32 devices in a mesh: mod: 4 (over y, x), seq: 8 (over z, core).
Axes of the slice: x: 2, y: 2, z: 4, core: 2. Of those that a mesh axis runs over, the one named last changes fastest.
Arguments:
- tokens: bfloat16 [2048, 4096], P(('mod', 'seq')), may hold values from -6 to 6
- norm_gain: float32 [3, 4096], replicated, may hold values from 0.2 to 2.6
- qkv_weight: bfloat16 [3, 4096, 12288], P(None, None, 'seq'), may hold values from -0.45 to 0.45
- out_weight: bfloat16 [3, 4096, 4096], P(None, 'seq'), may hold values from -0.375 to 0.375
- modality: int32 [16], replicated, may hold values from 0 to 2
- doc_lengths: int32 [4], replicated, may hold values from 1 to 1024, 2048 in all
Outputs:
- mixed: bfloat16 [2048, 4096], P(('mod', 'seq'))
The draws below stay inside these ranges and needn't reach their ends.
Inputs may be any that keep to these rules, and one draw needn't show every extreme that they name: `doc_lengths`: the lengths sum to 2048; documents follow one another from position 0 in the given order.
All inputs are finite; a program needn't handle non-finite values.
Results may differ from the reference program's by a relative error of at most 0.015.
Values may be sent and summed in bfloat16 or wider, within the bound.
A program may use at most 128 MiB of HBM per device.

```python
import math
import jax
import jax.numpy as jnp
import numpy as np
from jax import lax

D = 4096
HEADS = 32
HDIM = 128
MODS = 3
DOCS = 4
BLOCK = 128
TOKENS = 2048
BLOCKS = 16
HEAD_DEV = 4
FEATS = 4096
N_SEQ = 8


def draw_norm_gain(key, part):
    normal_draw = jax.random.uniform(jax.random.fold_in(key, 1), (MODS, D), jnp.float32, 0.6, 1.5)
    return normal_draw


def draw_qkv_weight(key, part):
    normal_draw = jax.random.normal(jax.random.fold_in(key, 3), (MODS, D, HEADS, 3, HDIM), jnp.float32)
    fan_scale = 1.0 / jnp.sqrt(jnp.float32(D))
    shared = normal_draw[:, :, :, 0:1, :] * 1.2 * fan_scale
    key_part = normal_draw[:, :, :, 1:2, :] * 1.2 * fan_scale
    values = normal_draw[:, :, :, 2:3, :] * fan_scale
    stacked = jnp.concatenate([shared, key_part, values], axis=3)
    return jnp.clip(stacked, -0.45, 0.45).reshape(MODS, D, HEADS * 3 * HDIM).astype(jnp.bfloat16)


def plant(values, rng, low, largest):
    spot = [jax.random.randint(jax.random.fold_in(rng, axis), (), 0, length) for axis, length in enumerate(values.shape)]
    widest = values.shape.index(max(values.shape))
    beside = spot[:widest] + [(spot[widest] + 1) % values.shape[widest]] + spot[widest + 1:]
    return values.at[tuple(spot)].set(low).at[tuple(beside)].set(largest)


def block_levels(key, dims, split, smallest, high):
    gain, own = 1.0, jax.random.fold_in(key, 6)
    for axis_at, blocks in split:
        draws = jnp.exp(jax.random.uniform(jax.random.fold_in(own, axis_at), (blocks,), jnp.float32, smallest / len(split), high / len(split)))
        gain = gain * jnp.repeat(draws, dims[axis_at] // blocks).reshape([-1 if axis == axis_at else 1 for axis in range(len(dims))])
    return gain


def rank_bounds(amount, slope):
    loads = [(1 << 20) // math.isqrt(grade ** slope) + 1 for grade in range(1, amount + 1)]
    spread = 1 + sum(loads) // (1 << 30)
    return np.cumsum(np.array([max(1, weight // spread) for weight in loads]))


def ranked(own_key, extent, amount, lean):
    grid = rank_bounds(amount, lean)
    lot = jax.random.randint(jax.random.fold_in(own_key, 1), extent, 0, int(grid[amount - 1]))
    grade = jnp.searchsorted(jnp.asarray(grid, jnp.int32), lot, side="right")
    return jax.random.permutation(jax.random.fold_in(own_key, 2), amount)[grade].astype(jnp.int32)


def profile(count, total, most, slope):
    weights = [(1 << 20) // math.isqrt(rank ** slope) + 1 for rank in range(2, count + 1)]
    surplus, counts = total - most - (count - 1), [1] * (count - 1)
    while surplus > 0:
        free = [i for i in range(count - 1) if counts[i] < most]
        whole, remaining = sum([weights[i] for i in free]), surplus
        for i in free:
            addition = min(most - counts[i], max(1, remaining * weights[i] // whole), surplus)
            counts[i] = counts[i] + addition
            surplus = surplus - addition
    return np.array([most] + counts)


def ragged_sizes(key, amount, total, limit, lean):
    if amount == 2:
        one = jax.random.randint(key, (), max(1, total - limit), min(limit, total - 1) + 1)
        return jnp.stack([one, total - one])
    sizes = jnp.asarray(profile(amount, total, limit, lean), jnp.int32)
    twos = (amount - 1) // 2
    donor, receiver = sizes[1:1 + 2 * twos:2], sizes[2:2 + 2 * twos:2]
    margin = jnp.minimum(donor - 1, limit - receiver)
    passed = jax.random.randint(jax.random.fold_in(key, 1), (twos,), 0, 1 << 20) % (margin + 1)
    sizes = sizes.at[1:1 + 2 * twos:2].set(donor - passed).at[2:2 + 2 * twos:2].set(receiver + passed)
    return sizes[jax.random.permutation(jax.random.fold_in(key, 2), amount)]


def scatter_about(rng, extent, deviation, limit, shards=(), kind=jnp.bfloat16):
    values = jax.random.normal(rng, extent, jnp.float32) * deviation
    if len(shards) > 0:
        values = block_levels(rng, extent, shards, -0.22, 0.18) * values
    return jnp.clip(values, min=-limit, max=limit).astype(kind)


def setup_inputs(seed: int = 0) -> dict:
    arg_keys = jax.random.split(jax.random.key(seed), 7)
    return {
        "tokens": scatter_about(arg_keys[0], (TOKENS, D), 1.0, 6.0, ((0, 32),)),
        "norm_gain": draw_norm_gain(jax.random.fold_in(arg_keys[6], 71), 0),
        "qkv_weight": draw_qkv_weight(jax.random.fold_in(arg_keys[6], 71), 0),
        "out_weight": scatter_about(arg_keys[3], (MODS, FEATS, D), (FEATS // 16) ** -0.5, 0.375, ((1, 8),)),
        "modality": plant(ranked(arg_keys[4], (BLOCKS,), MODS, 2), jax.random.fold_in(arg_keys[4], 3), 0, MODS - 1).astype(jnp.int32),
        "doc_lengths": ragged_sizes(arg_keys[5], DOCS, TOKENS, TOKENS // 2, 1).astype(jnp.int32),
    }


def reference(tokens, norm_gain, qkv_weight, out_weight, modality, doc_lengths):
    block_rows = tokens.reshape(BLOCKS, BLOCK, D).astype(jnp.float32)
    gain_rows = norm_gain[modality.astype(jnp.int32)]
    mean_square = lax.optimization_barrier(jnp.mean(block_rows * block_rows, axis=2, keepdims=True))
    normed = (block_rows * lax.rsqrt(mean_square + 1e-05) * gain_rows[:, None, :]).astype(jnp.bfloat16)

    def project(block_pair):
        row_block, block_mode = block_pair
        weight = lax.dynamic_index_in_dim(qkv_weight, block_mode, 0, keepdims=False)
        return jnp.dot(row_block, weight, preferred_element_type=jnp.float32).astype(jnp.bfloat16)
    projected = lax.map(project, (normed, modality))
    heads_first = jnp.moveaxis(projected.reshape(TOKENS, HEADS, 3, HDIM), 1, 0)
    doc_ends = jnp.cumsum(doc_lengths).astype(jnp.int32)
    position = jnp.arange(TOKENS, dtype=jnp.int32)
    document = lax.optimization_barrier(jnp.sum((position[:, None] >= doc_ends[None, :]).astype(jnp.int32), axis=1))
    allowed = (position[None, :] <= position[:, None]) & (document[None, :] == document[:, None])
    score_scale = 1.0 / math.sqrt(HDIM)

    def attend(one_head):
        scores = jnp.dot(one_head[:, 0, :], one_head[:, 1, :].T, preferred_element_type=jnp.float32) * score_scale
        row_max = lax.optimization_barrier(jnp.max(jnp.where(allowed, scores, -1e+30), axis=1, keepdims=True))
        weights = jnp.where(allowed, jnp.exp(scores - row_max), 0.0)
        totals = lax.optimization_barrier(jnp.sum(weights, axis=1, keepdims=True))
        summed = jnp.dot(weights.astype(jnp.bfloat16), one_head[:, 2, :], preferred_element_type=jnp.float32)
        return (summed / totals).astype(jnp.bfloat16)
    attended = lax.map(attend, heads_first)
    merged = jnp.moveaxis(attended, 0, 1).reshape(BLOCKS, BLOCK, N_SEQ, HEAD_DEV * HDIM)

    def output(block_pair):
        row_block, block_mode = block_pair
        weight = lax.dynamic_index_in_dim(out_weight, block_mode, 0, keepdims=False)
        weight = weight.reshape(N_SEQ, HEAD_DEV * HDIM, D).astype(jnp.float32)
        parts = jnp.einsum('bgc,gcd->gbd', row_block.astype(jnp.float32), weight)
        rounded = lax.optimization_barrier(parts.astype(jnp.bfloat16))
        return lax.optimization_barrier(jnp.sum(rounded.astype(jnp.float32), axis=0))
    projected_back = lax.map(output, (merged, modality)).reshape(TOKENS, D)
    return (tokens.astype(jnp.float32) + projected_back).astype(jnp.bfloat16)
```

```python
import functools
import math

import jax
import jax.numpy as jnp
from jax import lax
from jax.experimental import pallas as pl
from jax.experimental.pallas import tpu as pltpu
from jax.sharding import PartitionSpec as P

HDIM = 128
MESH = pl.DeviceIdType.MESH
F32 = jnp.float32
BF16 = jnp.bfloat16
LINES = 4
PIECES = 4
HALVES = 2
TILES = 2


def mul(x, k):
    return pl.multiple_of(x, k)


def remote(src, dst, send, recv, dev):
    return pltpu.make_async_remote_copy(
        src_ref=src, dst_ref=dst, send_sem=send, recv_sem=recv,
        device_id=dev, device_id_type=MESH,
    )


def greet(devs):
    barrier = pltpu.get_barrier_semaphore()
    for dev in devs:
        pl.semaphore_signal(barrier, inc=1, device_id=dev, device_id_type=MESH)
    pl.semaphore_wait(barrier, len(devs))


def sublayer(
    n, modality, doc_lengths, tokens, gain, w_hbm, o_hbm, out,
    wv, xg, stage, q_out, kv_out, att, pairbuf, bias, right_in, left_in,
    w_sem, o_sem, own_s, fs, fr, ps, pr, a_s, a_r, b_s, b_r, ps2, pr2, rs, rr, ls, lr,
):
    m = lax.axis_index("mod")
    s = lax.axis_index("seq")
    chip, core = s // 2, s % 2
    rows, width = tokens.shape
    pair = 2 * rows
    group = n * pair
    half = n // 2
    feats = q_out.shape[1]
    heads = feats // HDIM
    mods = w_hbm.shape[0]
    right = (m, ((chip + 1) % n) * 2 + core)
    left = (m, ((chip + n - 1) % n) * 2 + core)
    partner = (m, chip * 2 + (1 - core))
    chunks = 2
    piece = rows // chunks

    w_copies = [pltpu.make_async_copy(w_hbm.at[k], wv.at[k], w_sem.at[k]) for k in range(mods)]
    for c in w_copies:
        c.start()

    values = tokens[...].astype(F32)
    inv = lax.rsqrt(jnp.mean(values * values, axis=1, keepdims=True) + 1e-05)
    row_gain = gain[pl.ds(modality[m * n + chip], 1), :]
    xg[pl.ds(mul(chip * pair + core * rows, rows), rows), :] = (values * inv * row_gain).astype(BF16)

    @pl.when(m < 2)
    def _():
        kv_out[pl.ds(0, group), :] = jnp.zeros((group, 2 * feats), BF16)

    @pl.when(m < 1)
    def _():
        kv_out[pl.ds(group, group), :] = jnp.zeros((group, 2 * feats), BF16)

    others = [((m + d) % 4, s) for d in range(1, 4)]
    greet([right, left, partner] + others)

    def ref(block, which, c):
        return xg.at[pl.ds(mul(block * pair + which * rows + c * piece, piece), piece), :]

    def to_partner(block, c):
        r = ref(block, core, c)
        return remote(r, r, ps.at[block, c], pr.at[block, c], partner)

    def from_partner(block, c):
        r = ref(block, 1 - core, c)
        return remote(r, r, ps.at[block, c], pr.at[block, c], partner)

    def onward(block, c, dev, sem):
        r = ref(block, core, c)
        return remote(r, r, sem, fr.at[block, c], dev)

    for c in range(chunks):
        @pl.when(chip < n - 1)
        def _(c=c):
            onward(chip, c, right, own_s.at[0, c]).start()

        @pl.when(chip > 0)
        def _(c=c):
            onward(chip, c, left, own_s.at[1, c]).start()
    for c in range(chunks):
        to_partner(chip, c).start()

    def handle(k, c):
        for sign, dev in ((-1, right), (1, left)):
            block = chip + sign * k
            following = chip - sign

            @pl.when((block >= 0) & (block < n))
            def _(block=block, following=following, dev=dev):
                onward(block, c, dev, fs.at[block, c]).wait_recv()

                @pl.when((following >= 0) & (following < n))
                def _():
                    onward(block, c, dev, fs.at[block, c]).start()

                to_partner(block, c).start()

    def settle():
        for c in range(chunks):
            @pl.when(chip < n - 1)
            def _(c=c):
                onward(chip, c, right, own_s.at[0, c]).wait_send()

            @pl.when(chip > 0)
            def _(c=c):
                onward(chip, c, left, own_s.at[1, c]).wait_send()

            for d in range(n):
                to_partner((chip + d) % n, c).wait_send()
            for k in range(1, n):
                for sign, dev in ((-1, right), (1, left)):
                    block = chip + sign * k
                    following = chip - sign

                    @pl.when((block >= 0) & (block < n) & (following >= 0) & (following < n))
                    def _(block=block, dev=dev, c=c):
                        onward(block, c, dev, fs.at[block, c]).wait_send()

    tile = 256 if (3 * feats) % 256 == 0 else 128
    upper = chip // half
    near_side = chip * (1 - upper) + (n - 1 - chip) * upper
    far_sign = 1 - 2 * upper

    def block_at(t):
        if t == 0:
            return chip
        step = (t + 1) // 2
        two = step if t % 2 == 0 else -step
        past = (t - 1 - 2 * near_side + 2 * n) // (2 * n)
        return chip + two * (1 - past) + far_sign * (t - near_side) * past

    def own_copies(t, r):
        pieces = 4 if t == n - 1 else 1
        size = pair // pieces

        def copies(seg_from, seg_to, send, recv, to):
            return [
                remote(
                    kv_out.at[pl.ds(mul(seg_from * group + r + p * size, size), size), :],
                    kv_out.at[pl.ds(mul(seg_to * group + r + p * size, size), size), :],
                    send.at[t + p], recv.at[t + p], (to, s),
                )
                for p in range(pieces)
            ]

        return {
            "near01": copies(2, 1, a_s, a_r, 1),
            "far02": copies(2, 0, b_s, b_r, 2),
            "far13": copies(2, 0, b_s, b_r, 3),
            "near23": copies(2, 1, a_s, a_r, 3),
            "near32": copies(0, 1, a_s, a_r, 2),
        }

    own_sends = (("near01", "far02"), ("far13",), ("near23",), ("near32",))
    arrivals = ((), ("near01",), ("near32", "far02"), ("near23",))

    plan = []
    forwarded = []

    def forward_to(count):
        for t in range(len(forwarded), count):
            forwarded.append(t)

            @pl.when(m == 3)
            def _(t=t):
                for came, goes in zip(plan[t]["far13"], plan[t]["near32"]):
                    came.wait_recv()
                    goes.start()

    def project():
        t = len(plan)
        block = block_at(t)
        r = mul(block * pair, pair)
        mode = modality[m * n + block]
        for c in range(chunks):
            from_partner(block, c).wait_recv()

        def one_tile(j, carry):
            cols = pl.ds(mul(j * tile, tile), tile)
            stage[:, cols] = jnp.dot(
                xg[pl.ds(r, pair), :], wv[mode, :, cols], preferred_element_type=F32
            ).astype(BF16)
            return carry

        lax.fori_loop(0, 3 * feats // tile, one_tile, 0)
        for h in range(heads):
            q_out[pl.ds(r, pair), pl.ds(h * HDIM, HDIM)] = stage[:, pl.ds(3 * h * HDIM, HDIM)]
            kv_out[pl.ds(mul(2 * group + r, pair), pair), pl.ds(2 * h * HDIM, 2 * HDIM)] = stage[
                :, pl.ds((3 * h + 1) * HDIM, 2 * HDIM)
            ]
        copies = own_copies(t, r)
        plan.append(copies)
        for who in range(3):
            @pl.when(m == who)
            def _(who=who):
                for name in own_sends[who]:
                    for c in copies[name]:
                        c.start()
        forward_to(t)

    for c in range(chunks - 1):
        handle(1, c)
    for c in w_copies:
        c.wait()
    project()
    handle(1, chunks - 1)
    project()
    for k in range(2, n):
        for c in range(chunks):
            handle(k, c)
        project()
    squares = width // feats
    o_copies = [
        pltpu.make_async_copy(
            o_hbm.at[k, :, pl.ds(c * feats, feats)],
            wv.at[k, pl.ds(c * feats, feats), pl.ds(0, feats)],
            o_sem.at[k * squares + c],
        )
        for c in range(squares) for k in range(mods)
    ]
    for c in o_copies:
        c.start()
    forward_to(n)
    settle()
    for who in range(4):
        @pl.when(m == who)
        def _(who=who):
            for copies in plan:
                for name in arrivals[who]:
                    for c in copies[name]:
                        c.wait_recv()

    q, kv = q_out, kv_out
    keys = 3 * group
    chunk = keys
    while chunk > 1536:
        chunk //= 2
    scale = math.log2(math.e) / math.sqrt(HDIM)
    first_key = (m - 2) * group
    def mine(t):
        return pl.ds(mul(t * pair + core * rows, rows), rows)

    def theirs(t):
        return pl.ds(mul(t * pair + (1 - core) * rows, rows), rows)

    waited = []

    def compute(t, off):
        r = mul(((chip + off + n) % n) * pair, pair)
        pos = m * group + r + lax.broadcasted_iota(jnp.int32, (pair, 1), 0)
        end = jnp.int32(0)
        start = jnp.zeros((pair, 1), jnp.int32)
        for d in range(doc_lengths.shape[0]):
            end = end + doc_lengths[d]
            start = jnp.where(pos >= end, end, start)
        for c0 in range(0, keys, chunk):
            key = first_key + c0 + lax.broadcasted_iota(jnp.int32, (pair, chunk), 1)
            bias[:, pl.ds(c0, chunk)] = jnp.where((key <= pos) & (key >= start), 0.0, -1e30)
        for h in range(heads):
            query = q[pl.ds(r, pair), pl.ds(h * HDIM, HDIM)]
            top = total = acc = None
            for c0 in reversed(range(0, keys, chunk)):
                k_part = kv[pl.ds(c0, chunk), pl.ds(2 * h * HDIM, HDIM)]
                v_part = kv[pl.ds(c0, chunk), pl.ds((2 * h + 1) * HDIM, HDIM)]
                scores = lax.dot_general(
                    query, k_part, (((1,), (1,)), ((), ())), preferred_element_type=F32
                ) * scale + bias[:, pl.ds(c0, chunk)]
                peak = jnp.max(scores, axis=1, keepdims=True)
                new_top = peak if top is None else jnp.maximum(top, peak)
                weights = jnp.exp2(scores - new_top)
                if chunk != keys:
                    weights = jnp.where(bias[:, pl.ds(c0, chunk)] < 0.0, 0.0, weights)
                row_sum = jnp.sum(weights, axis=1, keepdims=True)
                added = jnp.dot(weights.astype(BF16), v_part, preferred_element_type=F32)
                if top is None:
                    total, acc = row_sum, added
                else:
                    fix = jnp.exp2(top - new_top)
                    total, acc = total * fix + row_sum, acc * fix + added
                top = new_top
            att[:, pl.ds(h * HDIM, HDIM)] = (acc / total).astype(BF16)
        if not waited:
            for c in o_copies:
                c.wait()
            waited.append(True)
        mode = modality[m * n + (chip + off + n) % n]

        def one_tile(j, carry):
            cols = pl.ds(mul(j * feats, feats), feats)
            square = wv[mode, cols, pl.ds(0, feats)]
            xg[pl.ds(t * pair, pair), cols] = jnp.dot(
                att[...], square, preferred_element_type=F32
            ).astype(BF16)
            return carry

        lax.fori_loop(0, squares, one_tile, 0)
        copy = remote(xg.at[theirs(t), :], pairbuf.at[t], ps2.at[t], pr2.at[t], partner)
        copy.start()
        return copy

    lo, hi = pl.ds(0, width // 2), pl.ds(width // 2, width // 2)
    sent = []

    def pair_sum(t, copy):
        copy.wait_recv()
        sent.append(copy)
        return xg[mine(t), :].astype(F32) + pairbuf[t].astype(F32)

    def send(src, dst, ss, rsm, dev):
        copy = remote(src, dst, ss, rsm, dev)
        copy.start()
        sent.append(copy)
        return copy

    copy = compute(0, half)
    xg[mine(0), :] = pair_sum(0, copy).astype(BF16)
    r_prev = send(xg.at[mine(0), lo], right_in.at[half - 1, :, lo], rs.at[half - 1], rr.at[half - 1], right)
    l_prev = send(xg.at[mine(0), hi], left_in.at[half - 1, :, hi], ls.at[half - 1], lr.at[half - 1], left)
    t = 1
    for k in range(half - 1, 0, -1):
        c_right = compute(t, k)
        c_left = compute(t + 1, -k)
        for which, (tt, c, prev, inbox, ss, rsm, dev, cols) in enumerate((
            (t, c_right, r_prev, right_in, rs, rr, right, lo),
            (t + 1, c_left, l_prev, left_in, ls, lr, left, hi),
        )):
            total = pair_sum(tt, c)
            prev.wait_recv()
            if k == half - 1:
                a, b = total[:, : width // 2], total[:, width // 2:]
                if which == 0:
                    a = a + inbox[k, :, lo].astype(F32)
                else:
                    b = b + inbox[k, :, hi].astype(F32)
                xg[mine(tt), lo] = a.astype(BF16)
                xg[mine(tt), hi] = b.astype(BF16)
            else:
                xg[mine(tt), :] = (total + inbox[k].astype(F32)).astype(BF16)
            new = send(xg.at[mine(tt), :], inbox.at[k - 1], ss.at[k - 1], rsm.at[k - 1], dev)
            if which == 0:
                r_prev = new
            else:
                l_prev = new
        t += 2
    c = compute(t, 0)
    total = pair_sum(t, c) + tokens[...].astype(F32)
    r_prev.wait_recv()
    total = total + right_in[0].astype(F32)
    l_prev.wait_recv()
    out[...] = (total + left_in[0].astype(F32)).astype(BF16)
    for copy in sent:
        copy.wait_send()


    for who in range(4):
        @pl.when(m == who)
        def _(who=who):
            for copies in plan:
                for name in own_sends[who]:
                    for c in copies[name]:
                        c.wait_send()


def body(n, tokens, norm_gain, qkv_weight, out_weight, modality, doc_lengths):
    rows, width = tokens.shape
    feats = out_weight.shape[1]
    mods = out_weight.shape[0]
    pair = 2 * rows
    group = n * pair
    half = n // 2
    vmem = pl.BlockSpec(memory_space=pltpu.VMEM)
    smem = pl.BlockSpec(memory_space=pltpu.SMEM)
    hbm = pl.BlockSpec(memory_space=pl.ANY)
    dma = pltpu.SemaphoreType.DMA
    limit = 62 * 1024 * 1024
    return pl.pallas_call(
        functools.partial(sublayer, n),
        out_shape=jax.ShapeDtypeStruct((rows, width), BF16),
        in_specs=[smem, smem, vmem, vmem, hbm, hbm],
        out_specs=vmem,
        scratch_shapes=[
            pltpu.VMEM((mods, width, 3 * feats), BF16),
            pltpu.VMEM((group, width), BF16),
            pltpu.VMEM((pair, 3 * feats), BF16),
            pltpu.VMEM((group, feats), BF16),
            pltpu.VMEM((3 * group, 2 * feats), BF16),
            pltpu.VMEM((pair, feats), BF16),
            pltpu.VMEM((n, rows, width), BF16),
            pltpu.VMEM((pair, 3 * group), F32),
            pltpu.VMEM((half, rows, width), BF16),
            pltpu.VMEM((half, rows, width), BF16),
            dma((mods,)), dma((mods * (width // feats),)),
            dma((2, 2)), dma((n, 2)), dma((n, 2)), dma((n, 2)), dma((n, 2)),
            dma((n + 3,)), dma((n + 3,)), dma((n + 3,)), dma((n + 3,)),
            dma((n,)), dma((n,)),
            dma((half,)), dma((half,)), dma((half,)), dma((half,)),
        ],
        compiler_params=pltpu.CompilerParams(
            collective_id=0, has_side_effects=True, vmem_limit_bytes=limit
        ),
    )(modality, doc_lengths, tokens, norm_gain, qkv_weight, out_weight)


def phased(
    n, modality, doc_lengths, tokens, gain, w_hbm, o_hbm, out,
    wq, wo, xg, stage, qkv, ao, ai, pb, rin, fin,
    w_sem, ys, other_s, fa, ne, po, fs, fr, ps, pr, qs, qr, as_, ar, bs, br, rs, rr, es, er,
):
    m = lax.axis_index("mod")
    s = lax.axis_index("seq")
    chip, core = s // 2, s % 2
    upper, parity = m // 2, m % 2
    across = (m + 2) % LINES
    rows, width = tokens.shape
    half = rows // 2
    pair = 2 * rows
    group = n * pair
    total_rows = LINES * group
    mods, feats, _ = o_hbm.shape
    share = qkv.shape[1]
    heads = share // (3 * HDIM)
    right = (m, ((chip + 1) % n) * 2 + core)
    left = (m, ((chip + n - 1) % n) * 2 + core)
    partner = (m, chip * 2 + (1 - core))
    hold = core == upper

    w_copies = [pltpu.make_async_copy(w_hbm.at[k], wq.at[k], w_sem.at[k]) for k in range(mods)]
    o_copies = [pltpu.make_async_copy(o_hbm.at[k], wo.at[k], w_sem.at[mods]) for k in range(mods)]
    for c in w_copies + o_copies:
        c.start()
    o_done = pltpu.make_async_copy(o_hbm, wo, w_sem.at[mods])

    barrier = pltpu.get_barrier_semaphore()
    known = [partner, (across, chip * 2 + (1 - core))]
    known += [((m + d) % LINES, s) for d in range(1, LINES)]
    for dev in known:
        pl.semaphore_signal(barrier, inc=1, device_id=dev, device_id_type=MESH)

    @pl.when(chip < n - 1)
    def _():
        pl.semaphore_signal(barrier, inc=1, device_id=right, device_id_type=MESH)

    @pl.when(chip > 0)
    def _():
        pl.semaphore_signal(barrier, inc=1, device_id=left, device_id_type=MESH)

    values = tokens[...].astype(F32)
    inv = lax.rsqrt(jnp.mean(values * values, axis=1, keepdims=True) + 1e-05)
    row_gain = gain[pl.ds(modality[m * n + chip], 1), :]
    normed = (values * inv * row_gain).astype(BF16)

    @pl.when(hold)
    def _():
        xg[upper, chip] = normed

    @pl.when(jnp.logical_not(hold))
    def _():
        out[...] = normed

    pl.semaphore_wait(barrier, len(known) + jnp.minimum(chip, 1) + jnp.minimum(n - 1 - chip, 1))

    def send(copy, cond=None):
        if cond is None:
            copy.start()
        else:
            pl.when(cond)(copy.start)

    def settled(ref, sem, cond=None):
        copy = remote(ref, ref, sem, fr.at[0, 0, 0], partner)
        if cond is None:
            copy.wait_send()
        else:
            pl.when(cond)(copy.wait_send)

    def arrive(copy, cond=None):
        if cond is None:
            copy.wait_recv()
        else:
            pl.when(cond)(copy.wait_recv)

    def strip(c):
        return pl.ds(c * (width // PIECES), width // PIECES)

    def part(k, block, which, c):
        return xg.at[k, block, pl.ds(mul(which * half, half), half), strip(c)]

    def along(k, block, c, dev, sem):
        r = part(k, block, core, c)
        return remote(r, r, sem, fr.at[k, block, c], dev)

    def to_partner(k, block, c, sem):
        r = part(k, block, core, c)
        return remote(r, r, sem, pr.at[k, block], partner)

    def from_partner(k, block):
        r = xg.at[k, block, pl.ds(mul((1 - core) * half, half), half), :]
        return remote(r, r, ps.at[k], pr.at[k, block], partner)

    moved = [
        remote(
            out.at[pl.ds(r * half, half), strip(c)], part(upper, chip, r, c),
            ys.at[0], fr.at[upper, chip, c], (across, chip * 2 + r),
        )
        for c in range(PIECES) for r in range(2)
    ]
    for copy in moved:
        pl.when(jnp.logical_not(hold))(copy.start)

    middle = n // 2
    beyond = chip // middle
    near_side = chip * (1 - beyond) + (n - 1 - chip) * beyond
    far_sign = 1 - 2 * beyond

    for c in range(PIECES):
        r = part(upper, chip, 1 - core, c)
        send(remote(r, r, other_s.at[0], fr.at[upper, chip, c], partner), hold)

    def unit_source(k):
        return (upper == k) & hold

    def enter_far(k, when, pieces=range(PIECES), both=False):
        source = unit_source(k)
        for c in pieces:
            arrive(along(k, chip, c, right, fa.at[k]), when & jnp.logical_not(source))
            send(along(k, chip, c, right, fa.at[k]), when & (beyond == 0))
            send(along(k, chip, c, left, fa.at[k]), when & (beyond == 1))
            if both:
                enter_near(k, when, (c,))
            send(to_partner(k, chip, c, po.at[k]), when & (source | (upper != k)))

    def enter_near(k, when, pieces=range(PIECES)):
        inner = when & (near_side > 0)
        for c in pieces:
            send(along(k, chip, c, left, ne.at[k]), inner & (beyond == 0))
            send(along(k, chip, c, right, ne.at[k]), inner & (beyond == 1))

    def handle(k, j, c, who=None):
        for sign, dev in ((-1, right), (1, left)):
            block = chip + sign * j
            following = chip - sign
            there = (block >= 0) & (block < n)
            if who is not None:
                there = there & (near_side > 0 if who == "inner" else near_side == 0)
            goes = there & (following >= 0) & (following < n)
            copy = along(k, block, c, dev, fs.at[k])
            arrive(copy, there)
            send(copy, goes)
            send(to_partner(k, block, c, ps.at[k]), there)

    def settle(k):
        unit = xg.at[k, 0, pl.ds(0, half), :]
        rest = xg.at[k, pl.ds(0, n - 1), pl.ds(0, half), :]
        inner = near_side > 0
        settled(unit, fa.at[k])
        settled(unit, ne.at[k], inner)
        settled(unit, po.at[k], unit_source(k) | (upper != k))
        settled(unit, other_s.at[0], hold & (upper == k))
        settled(rest, fs.at[k], inner)
        settled(rest, ps.at[k])

    def block_at(t):
        if t == 0:
            return chip
        step = (t + 1) // 2
        two = far_sign * (step if t % 2 == 1 else -step)
        past = (t - 1 - 2 * near_side + 2 * n) // (2 * n)
        return chip + two * (1 - past) + far_sign * (t - near_side) * past

    def order(t):
        return block_at(n - 1 - t)

    def place(line, k, block):
        at = ((2 * k + line % 2) * n + block) * pair + (line // 2) * rows
        return pl.ds(mul(at, rows), rows)

    def mode_of(k, block):
        return modality[(2 * k + parity) * n + block]

    def give(k, t, block, to):
        return remote(
            stage.at[t, to], qkv.at[place(m, k, block), :], qs.at[k, t], qr.at[k], (to, s)
        )

    def project(k, t, hold_back=False):
        block = block_at(t)
        if t > 0:
            from_partner(k, block).wait_recv()
        else:
            pl.when(jnp.logical_not(unit_source(k)))(from_partner(k, block).wait_recv)
        if k == 1:
            settled(stage.at[t, pl.ds(0, LINES - 1)], qs.at[0, t])
        mode = mode_of(k, block)
        per = LINES // TILES
        tile = per * share

        def one_tile(i, carry):
            j = (i + 1 + m // per) % TILES
            cols = pl.ds(mul(j * tile, 128), tile)
            got = jnp.dot(xg[k, block], wq[mode, :, cols], preferred_element_type=F32).astype(BF16)
            for i in range(per):
                to = j * per + i
                stage[t, to] = got[:, i * share:(i + 1) * share]
                if not hold_back:
                    pl.when(to != m)(give(k, t, block, to).start)
            return carry

        lax.fori_loop(0, TILES, one_tile, 0)
        qkv[place(m, k, block), :] = stage[t, m]

    def give_back(k, t):
        for off in range(1, LINES):
            give(k, t, block_at(t), (m + off) % LINES).start()

    def gathered(k):
        r = qkv.at[pl.ds(0, n * (LINES - 1) * rows), :]
        remote(r, r, qs.at[k, 0], qr.at[k], partner).wait_recv()

    scale = math.log2(math.e) / math.sqrt(HDIM)
    look = total_rows // 2

    def attend(k, t):
        block = order(t)
        for a in range(2):
            q0 = mul(((2 * k + a) * n + block) * pair, pair)
            if k == 0:
                k0, span = 0, (a + 1) * group
            else:
                k0, span = mul(q0 - look, pair), look + pair
            pos = q0 + lax.broadcasted_iota(jnp.int32, (pair, 1), 0)
            end = jnp.int32(0)
            start = jnp.zeros((pair, 1), jnp.int32)
            for d in range(doc_lengths.shape[0]):
                end = end + doc_lengths[d]
                start = jnp.where(pos >= end, end, start)
            key = k0 + lax.broadcasted_iota(jnp.int32, (pair, span), 1)
            allowed = (key <= pos) & (key >= start)
            for h in range(heads):
                base = 3 * h * HDIM
                query = qkv[pl.ds(q0, pair), pl.ds(base, HDIM)]
                keys = qkv[pl.ds(k0, span), pl.ds(base + HDIM, HDIM)]
                vals = qkv[pl.ds(k0, span), pl.ds(base + 2 * HDIM, HDIM)]
                scores = lax.dot_general(
                    query, keys, (((1,), (1,)), ((), ())), preferred_element_type=F32
                ) * scale
                scores = jnp.where(allowed, scores, -1e30)
                weights = jnp.exp2(scores - jnp.max(scores, axis=1, keepdims=True))
                row_sum = jnp.sum(weights, axis=1, keepdims=True)
                acc = jnp.dot(weights.astype(BF16), vals, preferred_element_type=F32)
                ao[pl.ds(q0, pair), pl.ds(h * HDIM, HDIM)] = (acc / row_sum).astype(BF16)
        for off in range(1, LINES):
            to = (m + off) % LINES
            send(remote(ao.at[place(to, k, block), :], ai.at[k, t, m], as_.at[k], ar.at[k, t], (to, s)))
        ai[k, t, m] = ao[place(m, k, block), :]

    def emit(k, t):
        block = order(t)
        r = ai.at[k, t, pl.ds(0, LINES - 1)]
        remote(r, r, as_.at[k], ar.at[k, t], partner).wait_recv()
        mode = mode_of(k, block)
        att = jnp.concatenate([ai[k, t, i] for i in range(LINES)], axis=1)
        tile = width // HALVES
        for j in range(HALVES):
            cols = pl.ds(j * tile, tile)
            xg[k, block, :, cols] = jnp.dot(att, wo[mode, :, cols], preferred_element_type=F32).astype(BF16)
            send(pair_copy(k, t, j))

    def pair_copy(k, t, c):
        cols = pl.ds(c * (width // HALVES), width // HALVES)
        r = xg.at[k, order(t), pl.ds(mul((1 - core) * half, half), half), cols]
        return remote(r, pb.at[k, t, :, cols], bs.at[k], br.at[k, t, c], partner)

    own_rows = pl.ds(mul(core * half, half), half)

    def inbox(k, slot, c):
        return rin.at[k, slot, :, strip(c)]

    def take(k, slot, c):
        r = inbox(k, slot, c)
        remote(r, r, rs.at[k], rr.at[k, slot, c], partner).wait_recv()

    def onward(k, block, c, rightward, leftward):
        r = xg.at[k, block, own_rows, strip(c)]
        send(
            remote(r, inbox(k, block, c), rs.at[k], rr.at[k, block, c], right),
            rightward,
        )
        slot = block + (n - block) * (1 - jnp.minimum(jnp.abs(chip - 1 - block), 1))
        send(
            remote(r, inbox(k, slot, c), rs.at[k], rr.at[k, slot, c], left),
            leftward,
        )

    def pair_wait(k, t, c):
        each = PIECES // HALVES
        if c % each == 0:
            pair_copy(k, t, c // each).wait_recv()

    def begin(k, t, c):
        block = order(t)

        @pl.when(near_side == 0)
        def _():
            pair_wait(k, t, c)
            xg[k, block, own_rows, strip(c)] = (
                xg[k, block, own_rows, strip(c)].astype(F32) + pb[k, t, :, strip(c)].astype(F32)
            ).astype(BF16)

        onward(k, block, c, chip == 0, chip == n - 1)

    def carry(k, t):
        block = order(t)
        inner = near_side > 0
        for c in range(PIECES):
            @pl.when(inner)
            def _():
                pair_wait(k, t, c)
                take(k, block, c)
                xg[k, block, own_rows, strip(c)] = (
                    xg[k, block, own_rows, strip(c)].astype(F32) + pb[k, t, :, strip(c)].astype(F32)
                    + rin[k, block, :, strip(c)].astype(F32)
                ).astype(BF16)

            onward(k, block, c, inner & (block > chip), inner & (block < chip))

    def finish(k):
        t = n - 1
        here = (upper == k) & hold
        away = jnp.logical_not(here)
        to = m + (across - m) * jnp.abs(upper - k)
        for c in range(PIECES):
            pair_wait(k, t, c)
            pl.when(chip > 0)(functools.partial(take, k, chip, c))
            pl.when(chip < n - 1)(functools.partial(take, k, n, c))
            total = xg[k, chip, own_rows, strip(c)].astype(F32) + pb[k, t, :, strip(c)].astype(F32)
            low = jnp.where(chip > 0, rin[k, chip, :, strip(c)].astype(F32), 0.0)
            high = jnp.where(chip < n - 1, rin[k, n, :, strip(c)].astype(F32), 0.0)
            total = total + low + high

            @pl.when(here)
            def _():
                out[own_rows, strip(c)] = (tokens[own_rows, strip(c)].astype(F32) + total).astype(BF16)

            @pl.when(away)
            def _():
                xg[k, chip, own_rows, strip(c)] = total.astype(BF16)

            send(
                remote(
                    xg.at[k, chip, own_rows, strip(c)], fin.at[own_rows, strip(c)],
                    es.at[k], er.at[core, c], (to, chip * 2 + upper),
                ), away,
            )

    def last(which, c):
        at = pl.ds(mul(which * half, half), half)
        r = fin.at[at, strip(c)]
        remote(r, r, es.at[0], er.at[which, c], partner).wait_recv()
        out[at, strip(c)] = (tokens[at, strip(c)].astype(F32) + fin[at, strip(c)].astype(F32)).astype(BF16)

    def many(k, j, who=None, part_of=range(PIECES)):
        for c in part_of:
            handle(k, j, c, who)

    def start(k, t):
        for c in range(PIECES):
            begin(k, t, c)

    first, second = range(PIECES // 2), range(PIECES // 2, PIECES)

    enter_far(1, upper == 1, first, both=True)
    enter_far(0, upper >= 0, both=True)
    many(0, 1)
    enter_far(1, upper == 0, first)
    enter_far(1, upper >= 0, second)
    for c in w_copies:
        c.wait()
    many(0, 2, "inner", first)
    project(0, 0)
    many(0, 2, "inner", second)
    enter_near(1, upper == 0, first)
    enter_near(1, upper >= 0, second)
    many(0, 2, "edge", first)
    project(0, 1)
    many(0, 2, "edge", second)
    many(1, 1, "inner")
    for t in range(2, n - 1):
        if t > 2:
            many(0, t)
        project(0, t)
    many(1, 2, "inner", first)
    many(0, n - 1)
    project(0, n - 1)
    many(1, 2, "inner", second)
    project(1, 0)
    o_done.wait()
    pl.when(jnp.logical_not(hold))(lambda: settled(out, ys.at[0]))
    settle(0)
    gathered(0)
    attend(0, 0)
    attend(0, 1)
    many(1, 1, "edge")
    project(1, 1, hold_back=True)
    many(1, 2, "edge")
    emit(0, 0)
    attend(0, 2)
    start(0, 0)
    emit(0, 1)
    for t in range(3, n):
        attend(0, t)
    give_back(1, 1)
    for u in range(2, n):
        if u + 1 < n:
            many(1, u + 1)
        project(1, u)
        if u == 2:
            start(0, 1)
    for t in range(2, n):
        emit(0, t)
        if t > 2:
            start(0, t - 1)
    settle(1)
    carry(0, 0)
    gathered(1)
    for t in range(n - 1):
        attend(1, t)
        if t > 0 and t < n - 2:
            carry(0, t)
    emit(1, 0)
    attend(1, n - 1)
    start(1, 0)
    carry(0, n - 2)
    emit(1, 1)
    for t in range(2, n):
        emit(1, t)
        start(1, t - 1)
    finish(0)
    for t in range(n - 1):
        carry(1, t)
    finish(1)

    @pl.when(hold)
    def _():
        for c in range(PIECES):
            last(1 - core, c)

    @pl.when(jnp.logical_not(hold))
    def _():
        for c in range(PIECES):
            for which in range(2):
                last(which, c)
    for k in range(2):
        if k == 1:
            for t in range(n):
                settled(stage.at[t, pl.ds(0, LINES - 1)], qs.at[k, t])
        back = ao.at[pl.ds(0, n * (LINES - 1) * rows), :]
        settled(back, as_.at[k])
        settled(pb.at[k], bs.at[k])
        settled(rin.at[k, pl.ds(0, n - 1)], rs.at[k])
        settled(xg.at[k, 0, pl.ds(0, half), :], es.at[k], jnp.logical_not(unit_source(k)))


def phased_body(n, tokens, norm_gain, qkv_weight, out_weight, modality, doc_lengths):
    rows, width = tokens.shape
    mods, feats, _ = out_weight.shape
    pair = 2 * rows
    share = 3 * feats // LINES
    vmem = pl.BlockSpec(memory_space=pltpu.VMEM)
    smem = pl.BlockSpec(memory_space=pltpu.SMEM)
    hbm = pl.BlockSpec(memory_space=pl.ANY)
    dma = pltpu.SemaphoreType.DMA
    return pl.pallas_call(
        functools.partial(phased, n),
        out_shape=jax.ShapeDtypeStruct((rows, width), BF16),
        in_specs=[smem, smem, vmem, vmem, hbm, hbm],
        out_specs=vmem,
        scratch_shapes=[
            pltpu.VMEM((mods, width, 3 * feats), BF16),
            pltpu.VMEM((mods, feats, width), BF16),
            pltpu.VMEM((2, n, rows, width), BF16),
            pltpu.VMEM((n, LINES, rows, share), BF16),
            pltpu.VMEM((LINES * n * pair, share), BF16),
            pltpu.VMEM((LINES * n * pair, share // 3), BF16),
            pltpu.VMEM((2, n, LINES, rows, share // 3), BF16),
            pltpu.VMEM((2, n, rows // 2, width), BF16),
            pltpu.VMEM((2, n + 1, rows // 2, width), BF16),
            pltpu.VMEM((rows, width), BF16),
            dma((mods + 1,)), dma((1,)), dma((1,)), dma((2,)), dma((2,)), dma((2,)),
            dma((2,)), dma((2, n, PIECES)), dma((2,)), dma((2, n)),
            dma((2, n)), dma((2,)), dma((2,)), dma((2, n)),
            dma((2,)), dma((2, n, HALVES)), dma((2,)), dma((2, n + 1, PIECES)),
            dma((2,)), dma((2, PIECES)),
        ],
        compiler_params=pltpu.CompilerParams(
            collective_id=0, has_side_effects=True, vmem_limit_bytes=67043328
        ),
    )(modality, doc_lengths, tokens, norm_gain, qkv_weight, out_weight)


def either(n, lines, tokens, norm_gain, qkv_weight, out_weight, modality, doc_lengths):
    heads = out_weight.shape[1] // HDIM
    fits = lines == LINES and heads % LINES == 0 and n % 2 == 0
    run = phased_body if fits else body
    return run(n, tokens, norm_gain, qkv_weight, out_weight, modality, doc_lengths)


def solution(mesh):
    return jax.shard_map(
        functools.partial(either, mesh.shape["seq"] // 2, mesh.shape["mod"]),
        mesh=mesh,
        in_specs=(
            P(("mod", "seq"), None),
            P(),
            P(None, None, "seq"),
            P(None, "seq", None),
            P(),
            P(),
        ),
        out_specs=P(("mod", "seq"), None),
        check_vma=False,
    )
```

```python
import functools
import math

import jax
import jax.numpy as jnp
from jax import lax
from jax.experimental import pallas as pl
from jax.experimental.pallas import tpu as pltpu
from jax.sharding import PartitionSpec as P

HDIM = 128
MESH = pl.DeviceIdType.MESH
F32 = jnp.float32
BF16 = jnp.bfloat16
LINES = 4
PIECES = 4
HALVES = 2
TILES = 2


def mul(x, k):
    return pl.multiple_of(x, k)


def remote(src, dst, send, recv, dev):
    return pltpu.make_async_remote_copy(
        src_ref=src, dst_ref=dst, send_sem=send, recv_sem=recv,
        device_id=dev, device_id_type=MESH,
    )


def greet(devs):
    barrier = pltpu.get_barrier_semaphore()
    for dev in devs:
        pl.semaphore_signal(barrier, inc=1, device_id=dev, device_id_type=MESH)
    pl.semaphore_wait(barrier, len(devs))


def sublayer(
    n, modality, doc_lengths, tokens, gain, w_hbm, o_hbm, out,
    wv, xg, stage, q_out, kv_out, att, pairbuf, bias, right_in, left_in,
    w_sem, o_sem, own_s, fs, fr, ps, pr, a_s, a_r, b_s, b_r, ps2, pr2, rs, rr, ls, lr,
):
    m = lax.axis_index("mod")
    s = lax.axis_index("seq")
    chip, core = s // 2, s % 2
    rows, width = tokens.shape
    pair = 2 * rows
    group = n * pair
    half = n // 2
    feats = q_out.shape[1]
    heads = feats // HDIM
    mods = w_hbm.shape[0]
    right = (m, ((chip + 1) % n) * 2 + core)
    left = (m, ((chip + n - 1) % n) * 2 + core)
    partner = (m, chip * 2 + (1 - core))
    chunks = 2
    piece = rows // chunks

    w_copies = [pltpu.make_async_copy(w_hbm.at[k], wv.at[k], w_sem.at[k]) for k in range(mods)]
    for c in w_copies:
        c.start()

    values = tokens[...].astype(F32)
    inv = lax.rsqrt(jnp.mean(values * values, axis=1, keepdims=True) + 1e-05)
    row_gain = gain[pl.ds(modality[m * n + chip], 1), :]
    xg[pl.ds(mul(chip * pair + core * rows, rows), rows), :] = (values * inv * row_gain).astype(BF16)

    @pl.when(m < 2)
    def _():
        kv_out[pl.ds(0, group), :] = jnp.zeros((group, 2 * feats), BF16)

    @pl.when(m < 1)
    def _():
        kv_out[pl.ds(group, group), :] = jnp.zeros((group, 2 * feats), BF16)

    others = [((m + d) % 4, s) for d in range(1, 4)]
    greet([right, left, partner] + others)

    def ref(block, which, c):
        return xg.at[pl.ds(mul(block * pair + which * rows + c * piece, piece), piece), :]

    def to_partner(block, c):
        r = ref(block, core, c)
        return remote(r, r, ps.at[block, c], pr.at[block, c], partner)

    def from_partner(block, c):
        r = ref(block, 1 - core, c)
        return remote(r, r, ps.at[block, c], pr.at[block, c], partner)

    def onward(block, c, dev, sem):
        r = ref(block, core, c)
        return remote(r, r, sem, fr.at[block, c], dev)

    for c in range(chunks):
        @pl.when(chip < n - 1)
        def _(c=c):
            onward(chip, c, right, own_s.at[0, c]).start()

        @pl.when(chip > 0)
        def _(c=c):
            onward(chip, c, left, own_s.at[1, c]).start()
    for c in range(chunks):
        to_partner(chip, c).start()

    def handle(k, c):
        for sign, dev in ((-1, right), (1, left)):
            block = chip + sign * k
            following = chip - sign

            @pl.when((block >= 0) & (block < n))
            def _(block=block, following=following, dev=dev):
                onward(block, c, dev, fs.at[block, c]).wait_recv()

                @pl.when((following >= 0) & (following < n))
                def _():
                    onward(block, c, dev, fs.at[block, c]).start()

                to_partner(block, c).start()

    def settle():
        for c in range(chunks):
            @pl.when(chip < n - 1)
            def _(c=c):
                onward(chip, c, right, own_s.at[0, c]).wait_send()

            @pl.when(chip > 0)
            def _(c=c):
                onward(chip, c, left, own_s.at[1, c]).wait_send()

            for d in range(n):
                to_partner((chip + d) % n, c).wait_send()
            for k in range(1, n):
                for sign, dev in ((-1, right), (1, left)):
                    block = chip + sign * k
                    following = chip - sign

                    @pl.when((block >= 0) & (block < n) & (following >= 0) & (following < n))
                    def _(block=block, dev=dev, c=c):
                        onward(block, c, dev, fs.at[block, c]).wait_send()

    tile = 256 if (3 * feats) % 256 == 0 else 128
    upper = chip // half
    near_side = chip * (1 - upper) + (n - 1 - chip) * upper
    far_sign = 1 - 2 * upper

    def block_at(t):
        if t == 0:
            return chip
        step = (t + 1) // 2
        two = step if t % 2 == 0 else -step
        past = (t - 1 - 2 * near_side + 2 * n) // (2 * n)
        return chip + two * (1 - past) + far_sign * (t - near_side) * past

    def own_copies(t, r):
        pieces = 4 if t == n - 1 else 1
        size = pair // pieces

        def copies(seg_from, seg_to, send, recv, to):
            return [
                remote(
                    kv_out.at[pl.ds(mul(seg_from * group + r + p * size, size), size), :],
                    kv_out.at[pl.ds(mul(seg_to * group + r + p * size, size), size), :],
                    send.at[t + p], recv.at[t + p], (to, s),
                )
                for p in range(pieces)
            ]

        return {
            "near01": copies(2, 1, a_s, a_r, 1),
            "far02": copies(2, 0, b_s, b_r, 2),
            "far13": copies(2, 0, b_s, b_r, 3),
            "near23": copies(2, 1, a_s, a_r, 3),
            "near32": copies(0, 1, a_s, a_r, 2),
        }

    own_sends = (("near01", "far02"), ("far13",), ("near23",), ("near32",))
    arrivals = ((), ("near01",), ("near32", "far02"), ("near23",))

    plan = []
    forwarded = []

    def forward_to(count):
        for t in range(len(forwarded), count):
            forwarded.append(t)

            @pl.when(m == 3)
            def _(t=t):
                for came, goes in zip(plan[t]["far13"], plan[t]["near32"]):
                    came.wait_recv()
                    goes.start()

    def project():
        t = len(plan)
        block = block_at(t)
        r = mul(block * pair, pair)
        mode = modality[m * n + block]
        for c in range(chunks):
            from_partner(block, c).wait_recv()

        def one_tile(j, carry):
            cols = pl.ds(mul(j * tile, tile), tile)
            stage[:, cols] = jnp.dot(
                xg[pl.ds(r, pair), :], wv[mode, :, cols], preferred_element_type=F32
            ).astype(BF16)
            return carry

        lax.fori_loop(0, 3 * feats // tile, one_tile, 0)
        for h in range(heads):
            q_out[pl.ds(r, pair), pl.ds(h * HDIM, HDIM)] = stage[:, pl.ds(3 * h * HDIM, HDIM)]
            kv_out[pl.ds(mul(2 * group + r, pair), pair), pl.ds(2 * h * HDIM, 2 * HDIM)] = stage[
                :, pl.ds((3 * h + 1) * HDIM, 2 * HDIM)
            ]
        copies = own_copies(t, r)
        plan.append(copies)
        for who in range(3):
            @pl.when(m == who)
            def _(who=who):
                for name in own_sends[who]:
                    for c in copies[name]:
                        c.start()
        forward_to(t)

    for c in range(chunks - 1):
        handle(1, c)
    for c in w_copies:
        c.wait()
    project()
    handle(1, chunks - 1)
    project()
    for k in range(2, n):
        for c in range(chunks):
            handle(k, c)
        project()
    squares = width // feats
    o_copies = [
        pltpu.make_async_copy(
            o_hbm.at[k, :, pl.ds(c * feats, feats)],
            wv.at[k, pl.ds(c * feats, feats), pl.ds(0, feats)],
            o_sem.at[k * squares + c],
        )
        for c in range(squares) for k in range(mods)
    ]
    for c in o_copies:
        c.start()
    forward_to(n)
    settle()
    for who in range(4):
        @pl.when(m == who)
        def _(who=who):
            for copies in plan:
                for name in arrivals[who]:
                    for c in copies[name]:
                        c.wait_recv()

    q, kv = q_out, kv_out
    keys = 3 * group
    chunk = keys
    while chunk > 1536:
        chunk //= 2
    scale = math.log2(math.e) / math.sqrt(HDIM)
    first_key = (m - 2) * group
    def mine(t):
        return pl.ds(mul(t * pair + core * rows, rows), rows)

    def theirs(t):
        return pl.ds(mul(t * pair + (1 - core) * rows, rows), rows)

    waited = []

    def compute(t, off):
        r = mul(((chip + off + n) % n) * pair, pair)
        pos = m * group + r + lax.broadcasted_iota(jnp.int32, (pair, 1), 0)
        end = jnp.int32(0)
        start = jnp.zeros((pair, 1), jnp.int32)
        for d in range(doc_lengths.shape[0]):
            end = end + doc_lengths[d]
            start = jnp.where(pos >= end, end, start)
        for c0 in range(0, keys, chunk):
            key = first_key + c0 + lax.broadcasted_iota(jnp.int32, (pair, chunk), 1)
            bias[:, pl.ds(c0, chunk)] = jnp.where((key <= pos) & (key >= start), 0.0, -1e30)
        for h in range(heads):
            query = q[pl.ds(r, pair), pl.ds(h * HDIM, HDIM)]
            top = total = acc = None
            for c0 in reversed(range(0, keys, chunk)):
                k_part = kv[pl.ds(c0, chunk), pl.ds(2 * h * HDIM, HDIM)]
                v_part = kv[pl.ds(c0, chunk), pl.ds((2 * h + 1) * HDIM, HDIM)]
                scores = lax.dot_general(
                    query, k_part, (((1,), (1,)), ((), ())), preferred_element_type=F32
                ) * scale + bias[:, pl.ds(c0, chunk)]
                peak = jnp.max(scores, axis=1, keepdims=True)
                new_top = peak if top is None else jnp.maximum(top, peak)
                weights = jnp.exp2(scores - new_top)
                if chunk != keys:
                    weights = jnp.where(bias[:, pl.ds(c0, chunk)] < 0.0, 0.0, weights)
                row_sum = jnp.sum(weights, axis=1, keepdims=True)
                added = jnp.dot(weights.astype(BF16), v_part, preferred_element_type=F32)
                if top is None:
                    total, acc = row_sum, added
                else:
                    fix = jnp.exp2(top - new_top)
                    total, acc = total * fix + row_sum, acc * fix + added
                top = new_top
            att[:, pl.ds(h * HDIM, HDIM)] = (acc / total).astype(BF16)
        if not waited:
            for c in o_copies:
                c.wait()
            waited.append(True)
        mode = modality[m * n + (chip + off + n) % n]

        def one_tile(j, carry):
            cols = pl.ds(mul(j * feats, feats), feats)
            square = wv[mode, cols, pl.ds(0, feats)]
            xg[pl.ds(t * pair, pair), cols] = jnp.dot(
                att[...], square, preferred_element_type=F32
            ).astype(BF16)
            return carry

        lax.fori_loop(0, squares, one_tile, 0)
        copy = remote(xg.at[theirs(t), :], pairbuf.at[t], ps2.at[t], pr2.at[t], partner)
        copy.start()
        return copy

    lo, hi = pl.ds(0, width // 2), pl.ds(width // 2, width // 2)
    sent = []

    def pair_sum(t, copy):
        copy.wait_recv()
        sent.append(copy)
        return xg[mine(t), :].astype(F32) + pairbuf[t].astype(F32)

    def send(src, dst, ss, rsm, dev):
        copy = remote(src, dst, ss, rsm, dev)
        copy.start()
        sent.append(copy)
        return copy

    copy = compute(0, half)
    xg[mine(0), :] = pair_sum(0, copy).astype(BF16)
    r_prev = send(xg.at[mine(0), lo], right_in.at[half - 1, :, lo], rs.at[half - 1], rr.at[half - 1], right)
    l_prev = send(xg.at[mine(0), hi], left_in.at[half - 1, :, hi], ls.at[half - 1], lr.at[half - 1], left)
    t = 1
    for k in range(half - 1, 0, -1):
        c_right = compute(t, k)
        c_left = compute(t + 1, -k)
        for which, (tt, c, prev, inbox, ss, rsm, dev, cols) in enumerate((
            (t, c_right, r_prev, right_in, rs, rr, right, lo),
            (t + 1, c_left, l_prev, left_in, ls, lr, left, hi),
        )):
            total = pair_sum(tt, c)
            prev.wait_recv()
            if k == half - 1:
                a, b = total[:, : width // 2], total[:, width // 2:]
                if which == 0:
                    a = a + inbox[k, :, lo].astype(F32)
                else:
                    b = b + inbox[k, :, hi].astype(F32)
                xg[mine(tt), lo] = a.astype(BF16)
                xg[mine(tt), hi] = b.astype(BF16)
            else:
                xg[mine(tt), :] = (total + inbox[k].astype(F32)).astype(BF16)
            new = send(xg.at[mine(tt), :], inbox.at[k - 1], ss.at[k - 1], rsm.at[k - 1], dev)
            if which == 0:
                r_prev = new
            else:
                l_prev = new
        t += 2
    c = compute(t, 0)
    total = pair_sum(t, c) + tokens[...].astype(F32)
    r_prev.wait_recv()
    total = total + right_in[0].astype(F32)
    l_prev.wait_recv()
    out[...] = (total + left_in[0].astype(F32)).astype(BF16)
    for copy in sent:
        copy.wait_send()


    for who in range(4):
        @pl.when(m == who)
        def _(who=who):
            for copies in plan:
                for name in own_sends[who]:
                    for c in copies[name]:
                        c.wait_send()


def body(n, tokens, norm_gain, qkv_weight, out_weight, modality, doc_lengths):
    rows, width = tokens.shape
    feats = out_weight.shape[1]
    mods = out_weight.shape[0]
    pair = 2 * rows
    group = n * pair
    half = n // 2
    vmem = pl.BlockSpec(memory_space=pltpu.VMEM)
    smem = pl.BlockSpec(memory_space=pltpu.SMEM)
    hbm = pl.BlockSpec(memory_space=pl.ANY)
    dma = pltpu.SemaphoreType.DMA
    limit = 62 * 1024 * 1024
    return pl.pallas_call(
        functools.partial(sublayer, n),
        out_shape=jax.ShapeDtypeStruct((rows, width), BF16),
        in_specs=[smem, smem, vmem, vmem, hbm, hbm],
        out_specs=vmem,
        scratch_shapes=[
            pltpu.VMEM((mods, width, 3 * feats), BF16),
            pltpu.VMEM((group, width), BF16),
            pltpu.VMEM((pair, 3 * feats), BF16),
            pltpu.VMEM((group, feats), BF16),
            pltpu.VMEM((3 * group, 2 * feats), BF16),
            pltpu.VMEM((pair, feats), BF16),
            pltpu.VMEM((n, rows, width), BF16),
            pltpu.VMEM((pair, 3 * group), F32),
            pltpu.VMEM((half, rows, width), BF16),
            pltpu.VMEM((half, rows, width), BF16),
            dma((mods,)), dma((mods * (width // feats),)),
            dma((2, 2)), dma((n, 2)), dma((n, 2)), dma((n, 2)), dma((n, 2)),
            dma((n + 3,)), dma((n + 3,)), dma((n + 3,)), dma((n + 3,)),
            dma((n,)), dma((n,)),
            dma((half,)), dma((half,)), dma((half,)), dma((half,)),
        ],
        compiler_params=pltpu.CompilerParams(
            collective_id=0, has_side_effects=True, vmem_limit_bytes=limit
        ),
    )(modality, doc_lengths, tokens, norm_gain, qkv_weight, out_weight)


def phased(
    n, modality, doc_lengths, tokens, gain, w_hbm, o_hbm, out,
    wq, wo, xg, stage, qkv, ao, ai, pb, rin, fin,
    w_sem, ys, other_s, fa, ne, po, fs, fr, ps, pr, qs, qr, as_, ar, bs, br, rs, rr, es, er,
):
    m = lax.axis_index("mod")
    s = lax.axis_index("seq")
    chip, core = s // 2, s % 2
    upper, parity = m // 2, m % 2
    across = (m + 2) % LINES
    rows, width = tokens.shape
    half = rows // 2
    pair = 2 * rows
    group = n * pair
    total_rows = LINES * group
    mods, feats, _ = o_hbm.shape
    share = qkv.shape[1]
    heads = share // (3 * HDIM)
    right = (m, ((chip + 1) % n) * 2 + core)
    left = (m, ((chip + n - 1) % n) * 2 + core)
    partner = (m, chip * 2 + (1 - core))
    hold = core == upper

    w_copies = [pltpu.make_async_copy(w_hbm.at[k], wq.at[k], w_sem.at[k]) for k in range(mods)]
    o_copies = [pltpu.make_async_copy(o_hbm.at[k], wo.at[k], w_sem.at[mods]) for k in range(mods)]
    for c in w_copies + o_copies:
        c.start()
    o_done = pltpu.make_async_copy(o_hbm, wo, w_sem.at[mods])

    barrier = pltpu.get_barrier_semaphore()
    known = [partner, (across, chip * 2 + (1 - core))]
    known += [((m + d) % LINES, s) for d in range(1, LINES)]
    for dev in known:
        pl.semaphore_signal(barrier, inc=1, device_id=dev, device_id_type=MESH)

    @pl.when(chip < n - 1)
    def _():
        pl.semaphore_signal(barrier, inc=1, device_id=right, device_id_type=MESH)

    @pl.when(chip > 0)
    def _():
        pl.semaphore_signal(barrier, inc=1, device_id=left, device_id_type=MESH)

    values = tokens[...].astype(F32)
    inv = lax.rsqrt(jnp.mean(values * values, axis=1, keepdims=True) + 1e-05)
    row_gain = gain[pl.ds(modality[m * n + chip], 1), :]
    normed = (values * inv * row_gain).astype(BF16)

    @pl.when(hold)
    def _():
        xg[upper, chip] = normed

    @pl.when(jnp.logical_not(hold))
    def _():
        out[...] = normed

    pl.semaphore_wait(barrier, len(known) + jnp.minimum(chip, 1) + jnp.minimum(n - 1 - chip, 1))

    def send(copy, cond=None):
        if cond is None:
            copy.start()
        else:
            pl.when(cond)(copy.start)

    def settled(ref, sem, cond=None):
        copy = remote(ref, ref, sem, fr.at[0, 0, 0], partner)
        if cond is None:
            copy.wait_send()
        else:
            pl.when(cond)(copy.wait_send)

    def arrive(copy, cond=None):
        if cond is None:
            copy.wait_recv()
        else:
            pl.when(cond)(copy.wait_recv)

    def strip(c):
        return pl.ds(c * (width // PIECES), width // PIECES)

    def part(k, block, which, c):
        return xg.at[k, block, pl.ds(mul(which * half, half), half), strip(c)]

    def along(k, block, c, dev, sem):
        r = part(k, block, core, c)
        return remote(r, r, sem, fr.at[k, block, c], dev)

    def to_partner(k, block, c, sem):
        r = part(k, block, core, c)
        return remote(r, r, sem, pr.at[k, block], partner)

    def from_partner(k, block):
        r = xg.at[k, block, pl.ds(mul((1 - core) * half, half), half), :]
        return remote(r, r, ps.at[k], pr.at[k, block], partner)

    moved = [
        remote(
            out.at[pl.ds(r * half, half), strip(c)], part(upper, chip, r, c),
            ys.at[0], fr.at[upper, chip, c], (across, chip * 2 + r),
        )
        for c in range(PIECES) for r in range(2)
    ]
    for copy in moved:
        pl.when(jnp.logical_not(hold))(copy.start)

    middle = n // 2
    beyond = chip // middle
    near_side = chip * (1 - beyond) + (n - 1 - chip) * beyond
    far_sign = 1 - 2 * beyond

    for c in range(PIECES):
        r = part(upper, chip, 1 - core, c)
        send(remote(r, r, other_s.at[0], fr.at[upper, chip, c], partner), hold)

    def unit_source(k):
        return (upper == k) & hold

    def enter_far(k, when, pieces=range(PIECES), both=False):
        source = unit_source(k)
        for c in pieces:
            arrive(along(k, chip, c, right, fa.at[k]), when & jnp.logical_not(source))
            send(along(k, chip, c, right, fa.at[k]), when & (beyond == 0))
            send(along(k, chip, c, left, fa.at[k]), when & (beyond == 1))
            if both:
                enter_near(k, when, (c,))
            send(to_partner(k, chip, c, po.at[k]), when & (source | (upper != k)))

    def enter_near(k, when, pieces=range(PIECES)):
        inner = when & (near_side > 0)
        for c in pieces:
            send(along(k, chip, c, left, ne.at[k]), inner & (beyond == 0))
            send(along(k, chip, c, right, ne.at[k]), inner & (beyond == 1))

    def handle(k, j, c, who=None):
        for sign, dev in ((-1, right), (1, left)):
            block = chip + sign * j
            following = chip - sign
            there = (block >= 0) & (block < n)
            if who is not None:
                there = there & (near_side > 0 if who == "inner" else near_side == 0)
            goes = there & (following >= 0) & (following < n)
            copy = along(k, block, c, dev, fs.at[k])
            arrive(copy, there)
            send(copy, goes)
            send(to_partner(k, block, c, ps.at[k]), there)

    def settle(k):
        unit = xg.at[k, 0, pl.ds(0, half), :]
        rest = xg.at[k, pl.ds(0, n - 1), pl.ds(0, half), :]
        inner = near_side > 0
        settled(unit, fa.at[k])
        settled(unit, ne.at[k], inner)
        settled(unit, po.at[k], unit_source(k) | (upper != k))
        settled(unit, other_s.at[0], hold & (upper == k))
        settled(rest, fs.at[k], inner)
        settled(rest, ps.at[k])

    def block_at(t):
        if t == 0:
            return chip
        step = (t + 1) // 2
        two = far_sign * (step if t % 2 == 1 else -step)
        past = (t - 1 - 2 * near_side + 2 * n) // (2 * n)
        return chip + two * (1 - past) + far_sign * (t - near_side) * past

    def order(t):
        return block_at(n - 1 - t)

    def place(line, k, block):
        at = ((2 * k + line % 2) * n + block) * pair + (line // 2) * rows
        return pl.ds(mul(at, rows), rows)

    def mode_of(k, block):
        return modality[(2 * k + parity) * n + block]

    def give(k, t, block, to):
        return remote(
            stage.at[t, to], qkv.at[place(m, k, block), :], qs.at[k, t], qr.at[k], (to, s)
        )

    def project(k, t, hold_back=False):
        block = block_at(t)
        if t > 0:
            from_partner(k, block).wait_recv()
        else:
            pl.when(jnp.logical_not(unit_source(k)))(from_partner(k, block).wait_recv)
        if k == 1:
            settled(stage.at[t, pl.ds(0, LINES - 1)], qs.at[0, t])
        mode = mode_of(k, block)
        per = LINES // TILES
        tile = per * share

        def one_tile(i, carry):
            j = (i + 1 + m // per) % TILES
            cols = pl.ds(mul(j * tile, 128), tile)
            got = jnp.dot(xg[k, block], wq[mode, :, cols], preferred_element_type=F32).astype(BF16)
            for i in range(per):
                to = j * per + i
                stage[t, to] = got[:, i * share:(i + 1) * share]
                if not hold_back:
                    pl.when(to != m)(give(k, t, block, to).start)
            return carry

        lax.fori_loop(0, TILES, one_tile, 0)
        qkv[place(m, k, block), :] = stage[t, m]

    def give_back(k, t):
        for off in range(1, LINES):
            give(k, t, block_at(t), (m + off) % LINES).start()

    def gathered(k):
        r = qkv.at[pl.ds(0, n * (LINES - 1) * rows), :]
        remote(r, r, qs.at[k, 0], qr.at[k], partner).wait_recv()

    scale = math.log2(math.e) / math.sqrt(HDIM)
    look = total_rows // 2

    def attend(k, t):
        block = order(t)
        for a in range(2):
            q0 = mul(((2 * k + a) * n + block) * pair, pair)
            if k == 0:
                k0, span = 0, (a + 1) * group
            else:
                k0, span = mul(q0 - look, pair), look + pair
            pos = q0 + lax.broadcasted_iota(jnp.int32, (pair, 1), 0)
            end = jnp.int32(0)
            start = jnp.zeros((pair, 1), jnp.int32)
            for d in range(doc_lengths.shape[0]):
                end = end + doc_lengths[d]
                start = jnp.where(pos >= end, end, start)
            key = k0 + lax.broadcasted_iota(jnp.int32, (pair, span), 1)
            allowed = (key <= pos) & (key >= start)
            for h in range(heads):
                base = 3 * h * HDIM
                query = qkv[pl.ds(q0, pair), pl.ds(base, HDIM)]
                keys = qkv[pl.ds(k0, span), pl.ds(base + HDIM, HDIM)]
                vals = qkv[pl.ds(k0, span), pl.ds(base + 2 * HDIM, HDIM)]
                scores = lax.dot_general(
                    query, keys, (((1,), (1,)), ((), ())), preferred_element_type=F32
                ) * scale
                scores = jnp.where(allowed, scores, -1e30)
                weights = jnp.exp2(scores - jnp.max(scores, axis=1, keepdims=True))
                row_sum = jnp.sum(weights, axis=1, keepdims=True)
                acc = jnp.dot(weights.astype(BF16), vals, preferred_element_type=F32)
                ao[pl.ds(q0, pair), pl.ds(h * HDIM, HDIM)] = (acc / row_sum).astype(BF16)
        for off in range(1, LINES):
            to = (m + off) % LINES
            send(remote(ao.at[place(to, k, block), :], ai.at[k, t, m], as_.at[k], ar.at[k, t], (to, s)))
        ai[k, t, m] = ao[place(m, k, block), :]

    def emit(k, t):
        block = order(t)
        r = ai.at[k, t, pl.ds(0, LINES - 1)]
        remote(r, r, as_.at[k], ar.at[k, t], partner).wait_recv()
        mode = mode_of(k, block)
        att = jnp.concatenate([ai[k, t, i] for i in range(LINES)], axis=1)
        tile = width // HALVES
        for j in range(HALVES):
            cols = pl.ds(j * tile, tile)
            xg[k, block, :, cols] = jnp.dot(att, wo[mode, :, cols], preferred_element_type=F32).astype(BF16)
            send(pair_copy(k, t, j))

    def pair_copy(k, t, c):
        cols = pl.ds(c * (width // HALVES), width // HALVES)
        r = xg.at[k, order(t), pl.ds(mul((1 - core) * half, half), half), cols]
        return remote(r, pb.at[k, t, :, cols], bs.at[k], br.at[k, t, c], partner)

    own_rows = pl.ds(mul(core * half, half), half)

    def inbox(k, slot, c):
        return rin.at[k, slot, :, strip(c)]

    def take(k, slot, c):
        r = inbox(k, slot, c)
        remote(r, r, rs.at[k], rr.at[k, slot, c], partner).wait_recv()

    def onward(k, block, c, rightward, leftward):
        r = xg.at[k, block, own_rows, strip(c)]
        send(
            remote(r, inbox(k, block, c), rs.at[k], rr.at[k, block, c], right),
            rightward,
        )
        slot = block + (n - block) * (1 - jnp.minimum(jnp.abs(chip - 1 - block), 1))
        send(
            remote(r, inbox(k, slot, c), rs.at[k], rr.at[k, slot, c], left),
            leftward,
        )

    def pair_wait(k, t, c):
        each = PIECES // HALVES
        if c % each == 0:
            pair_copy(k, t, c // each).wait_recv()

    def begin(k, t, c):
        block = order(t)

        @pl.when(near_side == 0)
        def _():
            pair_wait(k, t, c)
            xg[k, block, own_rows, strip(c)] = (
                xg[k, block, own_rows, strip(c)].astype(F32) + pb[k, t, :, strip(c)].astype(F32)
            ).astype(BF16)

        onward(k, block, c, chip == 0, chip == n - 1)

    def carry(k, *steps):
        inner = near_side > 0
        for c in range(PIECES):
            for t in steps:
                block = order(t)

                @pl.when(inner)
                def _():
                    pair_wait(k, t, c)
                    take(k, block, c)
                    xg[k, block, own_rows, strip(c)] = (
                        xg[k, block, own_rows, strip(c)].astype(F32) + pb[k, t, :, strip(c)].astype(F32)
                        + rin[k, block, :, strip(c)].astype(F32)
                    ).astype(BF16)

                onward(k, block, c, inner & (block > chip), inner & (block < chip))

    def finish(k):
        t = n - 1
        here = (upper == k) & hold
        away = jnp.logical_not(here)
        to = m + (across - m) * jnp.abs(upper - k)
        for c in range(PIECES):
            pair_wait(k, t, c)
            pl.when(chip > 0)(functools.partial(take, k, chip, c))
            pl.when(chip < n - 1)(functools.partial(take, k, n, c))
            total = xg[k, chip, own_rows, strip(c)].astype(F32) + pb[k, t, :, strip(c)].astype(F32)
            low = jnp.where(chip > 0, rin[k, chip, :, strip(c)].astype(F32), 0.0)
            high = jnp.where(chip < n - 1, rin[k, n, :, strip(c)].astype(F32), 0.0)
            total = total + low + high

            @pl.when(here)
            def _():
                out[own_rows, strip(c)] = (tokens[own_rows, strip(c)].astype(F32) + total).astype(BF16)

            @pl.when(away)
            def _():
                xg[k, chip, own_rows, strip(c)] = total.astype(BF16)

            send(
                remote(
                    xg.at[k, chip, own_rows, strip(c)], fin.at[own_rows, strip(c)],
                    es.at[k], er.at[core, c], (to, chip * 2 + upper),
                ), away,
            )

    def last(which, c):
        at = pl.ds(mul(which * half, half), half)
        r = fin.at[at, strip(c)]
        remote(r, r, es.at[0], er.at[which, c], partner).wait_recv()
        out[at, strip(c)] = (tokens[at, strip(c)].astype(F32) + fin[at, strip(c)].astype(F32)).astype(BF16)

    def many(k, j, who=None, part_of=range(PIECES)):
        for c in part_of:
            handle(k, j, c, who)

    def start(k, t):
        for c in range(PIECES):
            begin(k, t, c)

    first, second = range(PIECES // 2), range(PIECES // 2, PIECES)

    enter_far(1, upper == 1, first, both=True)
    enter_far(0, upper >= 0, both=True)
    many(0, 1)
    enter_far(1, upper == 0, first)
    enter_far(1, upper >= 0, second)
    for c in w_copies:
        c.wait()
    many(0, 2, "inner", first)
    project(0, 0)
    many(0, 2, "inner", second)
    enter_near(1, upper == 0, first)
    enter_near(1, upper >= 0, second)
    many(0, 2, "edge", first)
    project(0, 1)
    many(0, 2, "edge", second)
    many(1, 1, "inner")
    for t in range(2, n - 1):
        if t > 2:
            many(0, t)
        project(0, t)
    many(1, 2, "inner", first)
    many(0, n - 1)
    project(0, n - 1)
    many(1, 2, "inner", second)
    project(1, 0)
    o_done.wait()
    pl.when(jnp.logical_not(hold))(lambda: settled(out, ys.at[0]))
    settle(0)
    many(1, 1, "edge")
    gathered(0)
    attend(0, 0)
    attend(0, 1)
    project(1, 1, hold_back=True)
    many(1, 2, "edge")
    emit(0, 0)
    attend(0, 2)
    start(0, 0)
    give_back(1, 1)
    for u in range(2, n - 1):
        project(1, u)
        many(1, u + 1)
    emit(0, 1)
    project(1, n - 1)
    start(0, 1)
    for t in range(3, n):
        attend(0, t)
    for t in range(2, n - 1):
        emit(0, t)
    settle(1)
    for t in range(2, n - 1):
        start(0, t)
    carry(0, 0)
    gathered(1)
    for t in range(n - 1):
        attend(1, t)
    emit(0, n - 1)
    carry(0, *range(1, n - 1))
    emit(1, 0)
    attend(1, n - 1)
    start(1, 0)
    emit(1, 1)
    for t in range(2, n):
        emit(1, t)
        start(1, t - 1)
    carry(1, 0)
    finish(0)
    carry(1, *range(1, n - 1))
    finish(1)

    @pl.when(hold)
    def _():
        for c in range(PIECES):
            last(1 - core, c)

    @pl.when(jnp.logical_not(hold))
    def _():
        for c in range(PIECES):
            for which in range(2):
                last(which, c)
    for k in range(2):
        if k == 1:
            for t in range(n):
                settled(stage.at[t, pl.ds(0, LINES - 1)], qs.at[k, t])
        back = ao.at[pl.ds(0, n * (LINES - 1) * rows), :]
        settled(back, as_.at[k])
        settled(pb.at[k], bs.at[k])
        settled(rin.at[k, pl.ds(0, n - 1)], rs.at[k])
        settled(xg.at[k, 0, pl.ds(0, half), :], es.at[k], jnp.logical_not(unit_source(k)))


def phased_body(n, tokens, norm_gain, qkv_weight, out_weight, modality, doc_lengths):
    rows, width = tokens.shape
    mods, feats, _ = out_weight.shape
    pair = 2 * rows
    share = 3 * feats // LINES
    vmem = pl.BlockSpec(memory_space=pltpu.VMEM)
    smem = pl.BlockSpec(memory_space=pltpu.SMEM)
    hbm = pl.BlockSpec(memory_space=pl.ANY)
    dma = pltpu.SemaphoreType.DMA
    return pl.pallas_call(
        functools.partial(phased, n),
        out_shape=jax.ShapeDtypeStruct((rows, width), BF16),
        in_specs=[smem, smem, vmem, vmem, hbm, hbm],
        out_specs=vmem,
        scratch_shapes=[
            pltpu.VMEM((mods, width, 3 * feats), BF16),
            pltpu.VMEM((mods, feats, width), BF16),
            pltpu.VMEM((2, n, rows, width), BF16),
            pltpu.VMEM((n, LINES, rows, share), BF16),
            pltpu.VMEM((LINES * n * pair, share), BF16),
            pltpu.VMEM((LINES * n * pair, share // 3), BF16),
            pltpu.VMEM((2, n, LINES, rows, share // 3), BF16),
            pltpu.VMEM((2, n, rows // 2, width), BF16),
            pltpu.VMEM((2, n + 1, rows // 2, width), BF16),
            pltpu.VMEM((rows, width), BF16),
            dma((mods + 1,)), dma((1,)), dma((1,)), dma((2,)), dma((2,)), dma((2,)),
            dma((2,)), dma((2, n, PIECES)), dma((2,)), dma((2, n)),
            dma((2, n)), dma((2,)), dma((2,)), dma((2, n)),
            dma((2,)), dma((2, n, HALVES)), dma((2,)), dma((2, n + 1, PIECES)),
            dma((2,)), dma((2, PIECES)),
        ],
        compiler_params=pltpu.CompilerParams(
            collective_id=0, has_side_effects=True, vmem_limit_bytes=67043328
        ),
    )(modality, doc_lengths, tokens, norm_gain, qkv_weight, out_weight)


def either(n, lines, tokens, norm_gain, qkv_weight, out_weight, modality, doc_lengths):
    heads = out_weight.shape[1] // HDIM
    fits = lines == LINES and heads % LINES == 0 and n % 2 == 0
    run = phased_body if fits else body
    return run(n, tokens, norm_gain, qkv_weight, out_weight, modality, doc_lengths)


def solution(mesh):
    return jax.shard_map(
        functools.partial(either, mesh.shape["seq"] // 2, mesh.shape["mod"]),
        mesh=mesh,
        in_specs=(
            P(("mod", "seq"), None),
            P(),
            P(None, None, "seq"),
            P(None, "seq", None),
            P(),
            P(),
        ),
        out_specs=P(("mod", "seq"), None),
        check_vma=False,
    )
```

```python
import functools
import math

import jax
import jax.numpy as jnp
from jax import lax
from jax.experimental import pallas as pl
from jax.experimental.pallas import tpu as pltpu
from jax.sharding import PartitionSpec as P

HDIM = 128
MESH = pl.DeviceIdType.MESH
F32 = jnp.float32
BF16 = jnp.bfloat16
LINES = 4
PIECES = 4
HALVES = 2
TILES = 2


def mul(x, k):
    return pl.multiple_of(x, k)


def remote(src, dst, send, recv, dev):
    return pltpu.make_async_remote_copy(
        src_ref=src, dst_ref=dst, send_sem=send, recv_sem=recv,
        device_id=dev, device_id_type=MESH,
    )


def greet(devs):
    barrier = pltpu.get_barrier_semaphore()
    for dev in devs:
        pl.semaphore_signal(barrier, inc=1, device_id=dev, device_id_type=MESH)
    pl.semaphore_wait(barrier, len(devs))


def sublayer(
    n, modality, doc_lengths, tokens, gain, w_hbm, o_hbm, out,
    wv, xg, stage, q_out, kv_out, att, pairbuf, bias, right_in, left_in,
    w_sem, o_sem, own_s, fs, fr, ps, pr, a_s, a_r, b_s, b_r, ps2, pr2, rs, rr, ls, lr,
):
    m = lax.axis_index("mod")
    s = lax.axis_index("seq")
    chip, core = s // 2, s % 2
    rows, width = tokens.shape
    pair = 2 * rows
    group = n * pair
    half = n // 2
    feats = q_out.shape[1]
    heads = feats // HDIM
    mods = w_hbm.shape[0]
    right = (m, ((chip + 1) % n) * 2 + core)
    left = (m, ((chip + n - 1) % n) * 2 + core)
    partner = (m, chip * 2 + (1 - core))
    chunks = 2
    piece = rows // chunks

    w_copies = [pltpu.make_async_copy(w_hbm.at[k], wv.at[k], w_sem.at[k]) for k in range(mods)]
    for c in w_copies:
        c.start()

    values = tokens[...].astype(F32)
    inv = lax.rsqrt(jnp.mean(values * values, axis=1, keepdims=True) + 1e-05)
    row_gain = gain[pl.ds(modality[m * n + chip], 1), :]
    xg[pl.ds(mul(chip * pair + core * rows, rows), rows), :] = (values * inv * row_gain).astype(BF16)

    @pl.when(m < 2)
    def _():
        kv_out[pl.ds(0, group), :] = jnp.zeros((group, 2 * feats), BF16)

    @pl.when(m < 1)
    def _():
        kv_out[pl.ds(group, group), :] = jnp.zeros((group, 2 * feats), BF16)

    others = [((m + d) % 4, s) for d in range(1, 4)]
    greet([right, left, partner] + others)

    def ref(block, which, c):
        return xg.at[pl.ds(mul(block * pair + which * rows + c * piece, piece), piece), :]

    def to_partner(block, c):
        r = ref(block, core, c)
        return remote(r, r, ps.at[block, c], pr.at[block, c], partner)

    def from_partner(block, c):
        r = ref(block, 1 - core, c)
        return remote(r, r, ps.at[block, c], pr.at[block, c], partner)

    def onward(block, c, dev, sem):
        r = ref(block, core, c)
        return remote(r, r, sem, fr.at[block, c], dev)

    for c in range(chunks):
        @pl.when(chip < n - 1)
        def _(c=c):
            onward(chip, c, right, own_s.at[0, c]).start()

        @pl.when(chip > 0)
        def _(c=c):
            onward(chip, c, left, own_s.at[1, c]).start()
    for c in range(chunks):
        to_partner(chip, c).start()

    def handle(k, c):
        for sign, dev in ((-1, right), (1, left)):
            block = chip + sign * k
            following = chip - sign

            @pl.when((block >= 0) & (block < n))
            def _(block=block, following=following, dev=dev):
                onward(block, c, dev, fs.at[block, c]).wait_recv()

                @pl.when((following >= 0) & (following < n))
                def _():
                    onward(block, c, dev, fs.at[block, c]).start()

                to_partner(block, c).start()

    def settle():
        for c in range(chunks):
            @pl.when(chip < n - 1)
            def _(c=c):
                onward(chip, c, right, own_s.at[0, c]).wait_send()

            @pl.when(chip > 0)
            def _(c=c):
                onward(chip, c, left, own_s.at[1, c]).wait_send()

            for d in range(n):
                to_partner((chip + d) % n, c).wait_send()
            for k in range(1, n):
                for sign, dev in ((-1, right), (1, left)):
                    block = chip + sign * k
                    following = chip - sign

                    @pl.when((block >= 0) & (block < n) & (following >= 0) & (following < n))
                    def _(block=block, dev=dev, c=c):
                        onward(block, c, dev, fs.at[block, c]).wait_send()

    tile = 256 if (3 * feats) % 256 == 0 else 128
    upper = chip // half
    near_side = chip * (1 - upper) + (n - 1 - chip) * upper
    far_sign = 1 - 2 * upper

    def block_at(t):
        if t == 0:
            return chip
        step = (t + 1) // 2
        two = step if t % 2 == 0 else -step
        past = (t - 1 - 2 * near_side + 2 * n) // (2 * n)
        return chip + two * (1 - past) + far_sign * (t - near_side) * past

    def own_copies(t, r):
        pieces = 4 if t == n - 1 else 1
        size = pair // pieces

        def copies(seg_from, seg_to, send, recv, to):
            return [
                remote(
                    kv_out.at[pl.ds(mul(seg_from * group + r + p * size, size), size), :],
                    kv_out.at[pl.ds(mul(seg_to * group + r + p * size, size), size), :],
                    send.at[t + p], recv.at[t + p], (to, s),
                )
                for p in range(pieces)
            ]

        return {
            "near01": copies(2, 1, a_s, a_r, 1),
            "far02": copies(2, 0, b_s, b_r, 2),
            "far13": copies(2, 0, b_s, b_r, 3),
            "near23": copies(2, 1, a_s, a_r, 3),
            "near32": copies(0, 1, a_s, a_r, 2),
        }

    own_sends = (("near01", "far02"), ("far13",), ("near23",), ("near32",))
    arrivals = ((), ("near01",), ("near32", "far02"), ("near23",))

    plan = []
    forwarded = []

    def forward_to(count):
        for t in range(len(forwarded), count):
            forwarded.append(t)

            @pl.when(m == 3)
            def _(t=t):
                for came, goes in zip(plan[t]["far13"], plan[t]["near32"]):
                    came.wait_recv()
                    goes.start()

    def project():
        t = len(plan)
        block = block_at(t)
        r = mul(block * pair, pair)
        mode = modality[m * n + block]
        for c in range(chunks):
            from_partner(block, c).wait_recv()

        def one_tile(j, carry):
            cols = pl.ds(mul(j * tile, tile), tile)
            stage[:, cols] = jnp.dot(
                xg[pl.ds(r, pair), :], wv[mode, :, cols], preferred_element_type=F32
            ).astype(BF16)
            return carry

        lax.fori_loop(0, 3 * feats // tile, one_tile, 0)
        for h in range(heads):
            q_out[pl.ds(r, pair), pl.ds(h * HDIM, HDIM)] = stage[:, pl.ds(3 * h * HDIM, HDIM)]
            kv_out[pl.ds(mul(2 * group + r, pair), pair), pl.ds(2 * h * HDIM, 2 * HDIM)] = stage[
                :, pl.ds((3 * h + 1) * HDIM, 2 * HDIM)
            ]
        copies = own_copies(t, r)
        plan.append(copies)
        for who in range(3):
            @pl.when(m == who)
            def _(who=who):
                for name in own_sends[who]:
                    for c in copies[name]:
                        c.start()
        forward_to(t)

    for c in range(chunks - 1):
        handle(1, c)
    for c in w_copies:
        c.wait()
    project()
    handle(1, chunks - 1)
    project()
    for k in range(2, n):
        for c in range(chunks):
            handle(k, c)
        project()
    squares = width // feats
    o_copies = [
        pltpu.make_async_copy(
            o_hbm.at[k, :, pl.ds(c * feats, feats)],
            wv.at[k, pl.ds(c * feats, feats), pl.ds(0, feats)],
            o_sem.at[k * squares + c],
        )
        for c in range(squares) for k in range(mods)
    ]
    for c in o_copies:
        c.start()
    forward_to(n)
    settle()
    for who in range(4):
        @pl.when(m == who)
        def _(who=who):
            for copies in plan:
                for name in arrivals[who]:
                    for c in copies[name]:
                        c.wait_recv()

    q, kv = q_out, kv_out
    keys = 3 * group
    chunk = keys
    while chunk > 1536:
        chunk //= 2
    scale = math.log2(math.e) / math.sqrt(HDIM)
    first_key = (m - 2) * group
    def mine(t):
        return pl.ds(mul(t * pair + core * rows, rows), rows)

    def theirs(t):
        return pl.ds(mul(t * pair + (1 - core) * rows, rows), rows)

    waited = []

    def compute(t, off):
        r = mul(((chip + off + n) % n) * pair, pair)
        pos = m * group + r + lax.broadcasted_iota(jnp.int32, (pair, 1), 0)
        end = jnp.int32(0)
        start = jnp.zeros((pair, 1), jnp.int32)
        for d in range(doc_lengths.shape[0]):
            end = end + doc_lengths[d]
            start = jnp.where(pos >= end, end, start)
        for c0 in range(0, keys, chunk):
            key = first_key + c0 + lax.broadcasted_iota(jnp.int32, (pair, chunk), 1)
            bias[:, pl.ds(c0, chunk)] = jnp.where((key <= pos) & (key >= start), 0.0, -1e30)
        for h in range(heads):
            query = q[pl.ds(r, pair), pl.ds(h * HDIM, HDIM)]
            top = total = acc = None
            for c0 in reversed(range(0, keys, chunk)):
                k_part = kv[pl.ds(c0, chunk), pl.ds(2 * h * HDIM, HDIM)]
                v_part = kv[pl.ds(c0, chunk), pl.ds((2 * h + 1) * HDIM, HDIM)]
                scores = lax.dot_general(
                    query, k_part, (((1,), (1,)), ((), ())), preferred_element_type=F32
                ) * scale + bias[:, pl.ds(c0, chunk)]
                peak = jnp.max(scores, axis=1, keepdims=True)
                new_top = peak if top is None else jnp.maximum(top, peak)
                weights = jnp.exp2(scores - new_top)
                if chunk != keys:
                    weights = jnp.where(bias[:, pl.ds(c0, chunk)] < 0.0, 0.0, weights)
                row_sum = jnp.sum(weights, axis=1, keepdims=True)
                added = jnp.dot(weights.astype(BF16), v_part, preferred_element_type=F32)
                if top is None:
                    total, acc = row_sum, added
                else:
                    fix = jnp.exp2(top - new_top)
                    total, acc = total * fix + row_sum, acc * fix + added
                top = new_top
            att[:, pl.ds(h * HDIM, HDIM)] = (acc / total).astype(BF16)
        if not waited:
            for c in o_copies:
                c.wait()
            waited.append(True)
        mode = modality[m * n + (chip + off + n) % n]

        def one_tile(j, carry):
            cols = pl.ds(mul(j * feats, feats), feats)
            square = wv[mode, cols, pl.ds(0, feats)]
            xg[pl.ds(t * pair, pair), cols] = jnp.dot(
                att[...], square, preferred_element_type=F32
            ).astype(BF16)
            return carry

        lax.fori_loop(0, squares, one_tile, 0)
        copy = remote(xg.at[theirs(t), :], pairbuf.at[t], ps2.at[t], pr2.at[t], partner)
        copy.start()
        return copy

    lo, hi = pl.ds(0, width // 2), pl.ds(width // 2, width // 2)
    sent = []

    def pair_sum(t, copy):
        copy.wait_recv()
        sent.append(copy)
        return xg[mine(t), :].astype(F32) + pairbuf[t].astype(F32)

    def send(src, dst, ss, rsm, dev):
        copy = remote(src, dst, ss, rsm, dev)
        copy.start()
        sent.append(copy)
        return copy

    copy = compute(0, half)
    xg[mine(0), :] = pair_sum(0, copy).astype(BF16)
    r_prev = send(xg.at[mine(0), lo], right_in.at[half - 1, :, lo], rs.at[half - 1], rr.at[half - 1], right)
    l_prev = send(xg.at[mine(0), hi], left_in.at[half - 1, :, hi], ls.at[half - 1], lr.at[half - 1], left)
    t = 1
    for k in range(half - 1, 0, -1):
        c_right = compute(t, k)
        c_left = compute(t + 1, -k)
        for which, (tt, c, prev, inbox, ss, rsm, dev, cols) in enumerate((
            (t, c_right, r_prev, right_in, rs, rr, right, lo),
            (t + 1, c_left, l_prev, left_in, ls, lr, left, hi),
        )):
            total = pair_sum(tt, c)
            prev.wait_recv()
            if k == half - 1:
                a, b = total[:, : width // 2], total[:, width // 2:]
                if which == 0:
                    a = a + inbox[k, :, lo].astype(F32)
                else:
                    b = b + inbox[k, :, hi].astype(F32)
                xg[mine(tt), lo] = a.astype(BF16)
                xg[mine(tt), hi] = b.astype(BF16)
            else:
                xg[mine(tt), :] = (total + inbox[k].astype(F32)).astype(BF16)
            new = send(xg.at[mine(tt), :], inbox.at[k - 1], ss.at[k - 1], rsm.at[k - 1], dev)
            if which == 0:
                r_prev = new
            else:
                l_prev = new
        t += 2
    c = compute(t, 0)
    total = pair_sum(t, c) + tokens[...].astype(F32)
    r_prev.wait_recv()
    total = total + right_in[0].astype(F32)
    l_prev.wait_recv()
    out[...] = (total + left_in[0].astype(F32)).astype(BF16)
    for copy in sent:
        copy.wait_send()


    for who in range(4):
        @pl.when(m == who)
        def _(who=who):
            for copies in plan:
                for name in own_sends[who]:
                    for c in copies[name]:
                        c.wait_send()


def body(n, tokens, norm_gain, qkv_weight, out_weight, modality, doc_lengths):
    rows, width = tokens.shape
    feats = out_weight.shape[1]
    mods = out_weight.shape[0]
    pair = 2 * rows
    group = n * pair
    half = n // 2
    vmem = pl.BlockSpec(memory_space=pltpu.VMEM)
    smem = pl.BlockSpec(memory_space=pltpu.SMEM)
    hbm = pl.BlockSpec(memory_space=pl.ANY)
    dma = pltpu.SemaphoreType.DMA
    limit = 62 * 1024 * 1024
    return pl.pallas_call(
        functools.partial(sublayer, n),
        out_shape=jax.ShapeDtypeStruct((rows, width), BF16),
        in_specs=[smem, smem, vmem, vmem, hbm, hbm],
        out_specs=vmem,
        scratch_shapes=[
            pltpu.VMEM((mods, width, 3 * feats), BF16),
            pltpu.VMEM((group, width), BF16),
            pltpu.VMEM((pair, 3 * feats), BF16),
            pltpu.VMEM((group, feats), BF16),
            pltpu.VMEM((3 * group, 2 * feats), BF16),
            pltpu.VMEM((pair, feats), BF16),
            pltpu.VMEM((n, rows, width), BF16),
            pltpu.VMEM((pair, 3 * group), F32),
            pltpu.VMEM((half, rows, width), BF16),
            pltpu.VMEM((half, rows, width), BF16),
            dma((mods,)), dma((mods * (width // feats),)),
            dma((2, 2)), dma((n, 2)), dma((n, 2)), dma((n, 2)), dma((n, 2)),
            dma((n + 3,)), dma((n + 3,)), dma((n + 3,)), dma((n + 3,)),
            dma((n,)), dma((n,)),
            dma((half,)), dma((half,)), dma((half,)), dma((half,)),
        ],
        compiler_params=pltpu.CompilerParams(
            collective_id=0, has_side_effects=True, vmem_limit_bytes=limit
        ),
    )(modality, doc_lengths, tokens, norm_gain, qkv_weight, out_weight)


def phased(
    n, modality, doc_lengths, tokens, gain, w_hbm, o_hbm, out,
    wq, wo, xg, stage, qkv, ao, ai, pb, rin, fin,
    w_sem, ys, other_s, fa, ne, po, fs, fr, ps, pr, qs, qr, as_, ar, bs, br, rs, rr, es, er,
):
    m = lax.axis_index("mod")
    s = lax.axis_index("seq")
    chip, core = s // 2, s % 2
    upper, parity = m // 2, m % 2
    across = (m + 2) % LINES
    rows, width = tokens.shape
    half = rows // 2
    pair = 2 * rows
    group = n * pair
    total_rows = LINES * group
    mods, feats, _ = o_hbm.shape
    share = qkv.shape[1]
    heads = share // (3 * HDIM)
    right = (m, ((chip + 1) % n) * 2 + core)
    left = (m, ((chip + n - 1) % n) * 2 + core)
    partner = (m, chip * 2 + (1 - core))
    hold = core == upper

    w_copies = [pltpu.make_async_copy(w_hbm.at[k], wq.at[k], w_sem.at[k]) for k in range(mods)]
    o_copies = [pltpu.make_async_copy(o_hbm.at[k], wo.at[k], w_sem.at[mods]) for k in range(mods)]
    for c in w_copies + o_copies:
        c.start()
    o_done = pltpu.make_async_copy(o_hbm, wo, w_sem.at[mods])

    barrier = pltpu.get_barrier_semaphore()
    known = [partner, (across, chip * 2 + (1 - core))]
    known += [((m + d) % LINES, s) for d in range(1, LINES)]
    for dev in known:
        pl.semaphore_signal(barrier, inc=1, device_id=dev, device_id_type=MESH)

    @pl.when(chip < n - 1)
    def _():
        pl.semaphore_signal(barrier, inc=1, device_id=right, device_id_type=MESH)

    @pl.when(chip > 0)
    def _():
        pl.semaphore_signal(barrier, inc=1, device_id=left, device_id_type=MESH)

    values = tokens[...].astype(F32)
    inv = lax.rsqrt(jnp.mean(values * values, axis=1, keepdims=True) + 1e-05)
    row_gain = gain[pl.ds(modality[m * n + chip], 1), :]
    normed = (values * inv * row_gain).astype(BF16)

    @pl.when(hold)
    def _():
        xg[upper, chip] = normed

    @pl.when(jnp.logical_not(hold))
    def _():
        out[...] = normed

    pl.semaphore_wait(barrier, len(known) + jnp.minimum(chip, 1) + jnp.minimum(n - 1 - chip, 1))

    def send(copy, cond=None):
        if cond is None:
            copy.start()
        else:
            pl.when(cond)(copy.start)

    def settled(ref, sem, cond=None):
        copy = remote(ref, ref, sem, fr.at[0, 0, 0], partner)
        if cond is None:
            copy.wait_send()
        else:
            pl.when(cond)(copy.wait_send)

    def arrive(copy, cond=None):
        if cond is None:
            copy.wait_recv()
        else:
            pl.when(cond)(copy.wait_recv)

    def strip(c):
        return pl.ds(c * (width // PIECES), width // PIECES)

    def part(k, block, which, c):
        return xg.at[k, block, pl.ds(mul(which * half, half), half), strip(c)]

    def along(k, block, c, dev, sem):
        r = part(k, block, core, c)
        return remote(r, r, sem, fr.at[k, block, c], dev)

    def to_partner(k, block, c, sem):
        r = part(k, block, core, c)
        return remote(r, r, sem, pr.at[k, block], partner)

    def from_partner(k, block):
        r = xg.at[k, block, pl.ds(mul((1 - core) * half, half), half), :]
        return remote(r, r, ps.at[k], pr.at[k, block], partner)

    moved = [
        remote(
            out.at[pl.ds(r * half, half), strip(c)], part(upper, chip, r, c),
            ys.at[0], fr.at[upper, chip, c], (across, chip * 2 + r),
        )
        for c in range(PIECES) for r in range(2)
    ]
    for copy in moved:
        pl.when(jnp.logical_not(hold))(copy.start)

    middle = n // 2
    beyond = chip // middle
    near_side = chip * (1 - beyond) + (n - 1 - chip) * beyond
    far_sign = 1 - 2 * beyond

    for c in range(PIECES):
        r = part(upper, chip, 1 - core, c)
        send(remote(r, r, other_s.at[0], fr.at[upper, chip, c], partner), hold)

    def unit_source(k):
        return (upper == k) & hold

    def enter_far(k, when, pieces=range(PIECES), both=False):
        source = unit_source(k)
        for c in pieces:
            arrive(along(k, chip, c, right, fa.at[k]), when & jnp.logical_not(source))
            send(along(k, chip, c, right, fa.at[k]), when & (beyond == 0))
            send(along(k, chip, c, left, fa.at[k]), when & (beyond == 1))
            if both:
                enter_near(k, when, (c,))
            send(to_partner(k, chip, c, po.at[k]), when & (source | (upper != k)))

    def enter_near(k, when, pieces=range(PIECES)):
        inner = when & (near_side > 0)
        for c in pieces:
            send(along(k, chip, c, left, ne.at[k]), inner & (beyond == 0))
            send(along(k, chip, c, right, ne.at[k]), inner & (beyond == 1))

    def handle(k, j, c, who=None):
        for sign, dev in ((-1, right), (1, left)):
            block = chip + sign * j
            following = chip - sign
            there = (block >= 0) & (block < n)
            if who is not None:
                there = there & (near_side > 0 if who == "inner" else near_side == 0)
            goes = there & (following >= 0) & (following < n)
            copy = along(k, block, c, dev, fs.at[k])
            arrive(copy, there)
            send(copy, goes)
            send(to_partner(k, block, c, ps.at[k]), there)

    def settle(k):
        unit = xg.at[k, 0, pl.ds(0, half), :]
        rest = xg.at[k, pl.ds(0, n - 1), pl.ds(0, half), :]
        inner = near_side > 0
        settled(unit, fa.at[k])
        settled(unit, ne.at[k], inner)
        settled(unit, po.at[k], unit_source(k) | (upper != k))
        settled(unit, other_s.at[0], hold & (upper == k))
        settled(rest, fs.at[k], inner)
        settled(rest, ps.at[k])

    def block_at(t):
        if t == 0:
            return chip
        step = (t + 1) // 2
        two = far_sign * (step if t % 2 == 1 else -step)
        past = (t - 1 - 2 * near_side + 2 * n) // (2 * n)
        return chip + two * (1 - past) + far_sign * (t - near_side) * past

    def order(t):
        return block_at(n - 1 - t)

    def place(line, k, block):
        at = ((2 * k + line % 2) * n + block) * pair + (line // 2) * rows
        return pl.ds(mul(at, rows), rows)

    def mode_of(k, block):
        return modality[(2 * k + parity) * n + block]

    def give(k, t, block, to):
        return remote(
            stage.at[t, to], qkv.at[place(m, k, block), :], qs.at[k, t], qr.at[k], (to, s)
        )

    def project(k, t, hold_back=False):
        block = block_at(t)
        if t > 0:
            from_partner(k, block).wait_recv()
        else:
            pl.when(jnp.logical_not(unit_source(k)))(from_partner(k, block).wait_recv)
        if k == 1:
            settled(stage.at[t, pl.ds(0, LINES - 1)], qs.at[0, t])
        mode = mode_of(k, block)
        per = LINES // TILES
        tile = per * share

        def one_tile(i, carry):
            j = (i + 1 + m // per) % TILES
            cols = pl.ds(mul(j * tile, 128), tile)
            got = jnp.dot(xg[k, block], wq[mode, :, cols], preferred_element_type=F32).astype(BF16)
            for i in range(per):
                to = j * per + i
                stage[t, to] = got[:, i * share:(i + 1) * share]
                if not hold_back:
                    pl.when(to != m)(give(k, t, block, to).start)
            return carry

        lax.fori_loop(0, TILES, one_tile, 0)
        qkv[place(m, k, block), :] = stage[t, m]

    def give_back(k, t):
        for off in range(1, LINES):
            give(k, t, block_at(t), (m + off) % LINES).start()

    def gathered(k):
        r = qkv.at[pl.ds(0, n * (LINES - 1) * rows), :]
        remote(r, r, qs.at[k, 0], qr.at[k], partner).wait_recv()

    scale = math.log2(math.e) / math.sqrt(HDIM)
    look = total_rows // 2

    def attend(k, t):
        block = order(t)
        for a in range(2):
            q0 = mul(((2 * k + a) * n + block) * pair, pair)
            if k == 0:
                k0, span = 0, (a + 1) * group
            else:
                k0, span = mul(q0 - look, pair), look + pair
            pos = q0 + lax.broadcasted_iota(jnp.int32, (pair, 1), 0)
            end = jnp.int32(0)
            start = jnp.zeros((pair, 1), jnp.int32)
            for d in range(doc_lengths.shape[0]):
                end = end + doc_lengths[d]
                start = jnp.where(pos >= end, end, start)
            key = k0 + lax.broadcasted_iota(jnp.int32, (pair, span), 1)
            allowed = (key <= pos) & (key >= start)
            for h in range(heads):
                base = 3 * h * HDIM
                query = qkv[pl.ds(q0, pair), pl.ds(base, HDIM)]
                keys = qkv[pl.ds(k0, span), pl.ds(base + HDIM, HDIM)]
                vals = qkv[pl.ds(k0, span), pl.ds(base + 2 * HDIM, HDIM)]
                scores = lax.dot_general(
                    query, keys, (((1,), (1,)), ((), ())), preferred_element_type=F32
                ) * scale
                scores = jnp.where(allowed, scores, -1e30)
                weights = jnp.exp2(scores - jnp.max(scores, axis=1, keepdims=True))
                row_sum = jnp.sum(weights, axis=1, keepdims=True)
                acc = jnp.dot(weights.astype(BF16), vals, preferred_element_type=F32)
                ao[pl.ds(q0, pair), pl.ds(h * HDIM, HDIM)] = (acc / row_sum).astype(BF16)
        for off in range(1, LINES):
            to = (m + off) % LINES
            send(remote(ao.at[place(to, k, block), :], ai.at[k, t, m], as_.at[k], ar.at[k, t], (to, s)))
        ai[k, t, m] = ao[place(m, k, block), :]

    def emit(k, t):
        block = order(t)
        r = ai.at[k, t, pl.ds(0, LINES - 1)]
        remote(r, r, as_.at[k], ar.at[k, t], partner).wait_recv()
        mode = mode_of(k, block)
        att = jnp.concatenate([ai[k, t, i] for i in range(LINES)], axis=1)
        tile = width // HALVES
        for j in range(HALVES):
            cols = pl.ds(j * tile, tile)
            xg[k, block, :, cols] = jnp.dot(att, wo[mode, :, cols], preferred_element_type=F32).astype(BF16)
            send(pair_copy(k, t, j))

    def pair_copy(k, t, c):
        cols = pl.ds(c * (width // HALVES), width // HALVES)
        r = xg.at[k, order(t), pl.ds(mul((1 - core) * half, half), half), cols]
        return remote(r, pb.at[k, t, :, cols], bs.at[k], br.at[k, t, c], partner)

    own_rows = pl.ds(mul(core * half, half), half)

    def inbox(k, slot, c):
        return rin.at[k, slot, :, strip(c)]

    def take(k, slot, c):
        r = inbox(k, slot, c)
        remote(r, r, rs.at[k], rr.at[k, slot, c], partner).wait_recv()

    def onward(k, block, c, rightward, leftward):
        r = xg.at[k, block, own_rows, strip(c)]
        send(
            remote(r, inbox(k, block, c), rs.at[k], rr.at[k, block, c], right),
            rightward,
        )
        slot = block + (n - block) * (1 - jnp.minimum(jnp.abs(chip - 1 - block), 1))
        send(
            remote(r, inbox(k, slot, c), rs.at[k], rr.at[k, slot, c], left),
            leftward,
        )

    def pair_wait(k, t, c):
        each = PIECES // HALVES
        if c % each == 0:
            pair_copy(k, t, c // each).wait_recv()

    def begin(k, t, c):
        block = order(t)

        @pl.when(near_side == 0)
        def _():
            pair_wait(k, t, c)
            xg[k, block, own_rows, strip(c)] = (
                xg[k, block, own_rows, strip(c)].astype(F32) + pb[k, t, :, strip(c)].astype(F32)
            ).astype(BF16)

        onward(k, block, c, chip == 0, chip == n - 1)

    def carry(k, *steps):
        inner = near_side > 0
        for c in range(PIECES):
            for t in steps:
                block = order(t)

                @pl.when(inner)
                def _():
                    pair_wait(k, t, c)
                    take(k, block, c)
                    xg[k, block, own_rows, strip(c)] = (
                        xg[k, block, own_rows, strip(c)].astype(F32) + pb[k, t, :, strip(c)].astype(F32)
                        + rin[k, block, :, strip(c)].astype(F32)
                    ).astype(BF16)

                onward(k, block, c, inner & (block > chip), inner & (block < chip))

    def finish(k):
        t = n - 1
        here = (upper == k) & hold
        away = jnp.logical_not(here)
        to = m + (across - m) * jnp.abs(upper - k)
        for c in range(PIECES):
            pair_wait(k, t, c)
            pl.when(chip > 0)(functools.partial(take, k, chip, c))
            pl.when(chip < n - 1)(functools.partial(take, k, n, c))
            total = xg[k, chip, own_rows, strip(c)].astype(F32) + pb[k, t, :, strip(c)].astype(F32)
            low = jnp.where(chip > 0, rin[k, chip, :, strip(c)].astype(F32), 0.0)
            high = jnp.where(chip < n - 1, rin[k, n, :, strip(c)].astype(F32), 0.0)
            total = total + low + high

            @pl.when(here)
            def _():
                out[own_rows, strip(c)] = (tokens[own_rows, strip(c)].astype(F32) + total).astype(BF16)

            @pl.when(away)
            def _():
                xg[k, chip, own_rows, strip(c)] = total.astype(BF16)

            send(
                remote(
                    xg.at[k, chip, own_rows, strip(c)], fin.at[own_rows, strip(c)],
                    es.at[k], er.at[core, c], (to, chip * 2 + upper),
                ), away,
            )

    def last(which, c):
        at = pl.ds(mul(which * half, half), half)
        r = fin.at[at, strip(c)]
        remote(r, r, es.at[0], er.at[which, c], partner).wait_recv()
        out[at, strip(c)] = (tokens[at, strip(c)].astype(F32) + fin[at, strip(c)].astype(F32)).astype(BF16)

    def many(k, j, who=None, part_of=range(PIECES)):
        for c in part_of:
            handle(k, j, c, who)

    def start(k, t):
        for c in range(PIECES):
            begin(k, t, c)

    first, second = range(PIECES // 2), range(PIECES // 2, PIECES)

    enter_far(1, upper == 1, first, both=True)
    enter_far(0, upper >= 0, both=True)
    many(0, 1)
    enter_far(1, upper == 0, first)
    enter_far(1, upper >= 0, second)
    for c in w_copies:
        c.wait()
    many(0, 2, "inner", first)
    project(0, 0)
    many(0, 2, "inner", second)
    enter_near(1, upper == 0, first)
    enter_near(1, upper >= 0, second)
    many(0, 2, "edge", first)
    project(0, 1)
    many(0, 2, "edge", second)
    many(1, 1, "inner")
    for t in range(2, n - 1):
        if t > 2:
            many(0, t)
        project(0, t)
    many(1, 2, "inner", first)
    many(0, n - 1)
    project(0, n - 1)
    many(1, 2, "inner", second)
    project(1, 0, hold_back=True)
    o_done.wait()
    pl.when(jnp.logical_not(hold))(lambda: settled(out, ys.at[0]))
    settle(0)
    many(1, 1, "edge")
    gathered(0)
    attend(0, 0)
    attend(0, 1)
    give_back(1, 0)
    project(1, 1, hold_back=True)
    many(1, 2, "edge")
    emit(0, 0)
    attend(0, 2)
    start(0, 0)
    give_back(1, 1)
    emit(0, 1)
    for u in range(2, n - 1):
        many(1, u + 1)
        project(1, u)
        if u == 2:
            start(0, 1)
    project(1, n - 1)
    for t in range(3, n):
        attend(0, t)
    for t in range(2, n - 1):
        emit(0, t)
    settle(1)
    for t in range(2, n - 1):
        start(0, t)
    carry(0, 0)
    gathered(1)
    for t in range(n - 1):
        attend(1, t)
    emit(0, n - 1)
    carry(0, *range(1, n - 1))
    emit(1, 0)
    attend(1, n - 1)
    start(1, 0)
    emit(1, 1)
    for t in range(2, n):
        emit(1, t)
        start(1, t - 1)
    carry(1, 0)
    finish(0)
    carry(1, *range(1, n - 1))
    finish(1)

    @pl.when(hold)
    def _():
        for c in range(PIECES):
            last(1 - core, c)

    @pl.when(jnp.logical_not(hold))
    def _():
        for c in range(PIECES):
            for which in range(2):
                last(which, c)
    for k in range(2):
        if k == 1:
            for t in range(n):
                settled(stage.at[t, pl.ds(0, LINES - 1)], qs.at[k, t])
        back = ao.at[pl.ds(0, n * (LINES - 1) * rows), :]
        settled(back, as_.at[k])
        settled(pb.at[k], bs.at[k])
        settled(rin.at[k, pl.ds(0, n - 1)], rs.at[k])
        settled(xg.at[k, 0, pl.ds(0, half), :], es.at[k], jnp.logical_not(unit_source(k)))


def phased_body(n, tokens, norm_gain, qkv_weight, out_weight, modality, doc_lengths):
    rows, width = tokens.shape
    mods, feats, _ = out_weight.shape
    pair = 2 * rows
    share = 3 * feats // LINES
    vmem = pl.BlockSpec(memory_space=pltpu.VMEM)
    smem = pl.BlockSpec(memory_space=pltpu.SMEM)
    hbm = pl.BlockSpec(memory_space=pl.ANY)
    dma = pltpu.SemaphoreType.DMA
    return pl.pallas_call(
        functools.partial(phased, n),
        out_shape=jax.ShapeDtypeStruct((rows, width), BF16),
        in_specs=[smem, smem, vmem, vmem, hbm, hbm],
        out_specs=vmem,
        scratch_shapes=[
            pltpu.VMEM((mods, width, 3 * feats), BF16),
            pltpu.VMEM((mods, feats, width), BF16),
            pltpu.VMEM((2, n, rows, width), BF16),
            pltpu.VMEM((n, LINES, rows, share), BF16),
            pltpu.VMEM((LINES * n * pair, share), BF16),
            pltpu.VMEM((LINES * n * pair, share // 3), BF16),
            pltpu.VMEM((2, n, LINES, rows, share // 3), BF16),
            pltpu.VMEM((2, n, rows // 2, width), BF16),
            pltpu.VMEM((2, n + 1, rows // 2, width), BF16),
            pltpu.VMEM((rows, width), BF16),
            dma((mods + 1,)), dma((1,)), dma((1,)), dma((2,)), dma((2,)), dma((2,)),
            dma((2,)), dma((2, n, PIECES)), dma((2,)), dma((2, n)),
            dma((2, n)), dma((2,)), dma((2,)), dma((2, n)),
            dma((2,)), dma((2, n, HALVES)), dma((2,)), dma((2, n + 1, PIECES)),
            dma((2,)), dma((2, PIECES)),
        ],
        compiler_params=pltpu.CompilerParams(
            collective_id=0, has_side_effects=True, vmem_limit_bytes=67043328
        ),
    )(modality, doc_lengths, tokens, norm_gain, qkv_weight, out_weight)


def either(n, lines, tokens, norm_gain, qkv_weight, out_weight, modality, doc_lengths):
    heads = out_weight.shape[1] // HDIM
    fits = lines == LINES and heads % LINES == 0 and n % 2 == 0
    run = phased_body if fits else body
    return run(n, tokens, norm_gain, qkv_weight, out_weight, modality, doc_lengths)


def solution(mesh):
    return jax.shard_map(
        functools.partial(either, mesh.shape["seq"] // 2, mesh.shape["mod"]),
        mesh=mesh,
        in_specs=(
            P(("mod", "seq"), None),
            P(),
            P(None, None, "seq"),
            P(None, "seq", None),
            P(),
            P(),
        ),
        out_specs=P(("mod", "seq"), None),
        check_vma=False,
    )
```
